128 devices in a mesh: seq: 8 (over x, core), tp: 16 (over y, z).
Axes of the slice: x: 4, y: 4, z: 4, core: 2. Of those that a mesh axis runs over, the one named last changes fastest.
Arguments:
- vit_input: bfloat16 [8192, 1280], P(('seq', 'tp')), may hold values from -6 to 6
- image_lengths: int32 [8, 2], P('seq'), may hold values from 1 to 192, 256 in all within a row
- positions: int32 [2048], replicated, may hold values from 0 to 2047, each once
- vit_ln_gain: float32 [1280], replicated, may hold values from 0.25 to 1.75
- w_qkv: bfloat16 [1280, 3, 1280], P(None, None, 'tp'), may hold values from -0.15625 to 0.15625
- w_proj: bfloat16 [1280, 1280], P('tp'), may hold values from -0.15625 to 0.15625
- merger_ln_gain: float32 [1280], replicated, may hold values from 0.25 to 1.75
- merger_w1: bfloat16 [5120, 5120], P(None, 'tp'), may hold values from -0.078125 to 0.078125
- merger_w2: bfloat16 [5120, 8192], P('tp'), may hold values from -0.36336105 to 0.36336105
- norm_gain: float32 [8192], P('seq'), may hold values from 0.25 to 1.75
- gate_up_weight: bfloat16 [8192, 2, 29568], P('seq', None, 'tp'), may hold values from -0.0625 to 0.0625
- down_weight: bfloat16 [29568, 8192], P('tp', 'seq'), may hold values from -0.125 to 0.125
Outputs:
- mixed: bfloat16 [2048, 8192], P('tp', 'seq')
The draws below stay inside these ranges and needn't reach their ends.
Inputs may be any that keep to these rules, and one draw needn't show every extreme that they name: `image_lengths`: each row sums to 256. `positions`: a permutation: every slot once.
All inputs are finite; a program needn't handle non-finite values.
Results may differ from the reference program's by a relative error of at most 0.038.
Values may be sent and summed in bfloat16 or wider, within the bound.
A program may use at most 128 MiB of HBM per device.

```python
import math
import jax
import jax.numpy as jnp
import numpy as np
from jax import lax

VW = 1280
HEADS = 16
D = 8192
FF = 29568
IMG_GROUP = 2
HD = 80
MW = 5120
GROUPS = 8
GROUP_TOK = 256
TOKENS = 2048
PATCHES = 8192
N_SEQ = 8
N_TP = 16


def draw_merger_w2(key, part):
    first = jax.random.fold_in(key, 11)
    second = jax.random.fold_in(key, 23)
    third = jax.random.fold_in(key, 37)
    base = jnp.clip(jax.random.normal(first, (MW, D), jnp.float32), -6.0, 6.0)
    column_place = jnp.arange(D, dtype=jnp.float32) / D
    rough = jnp.exp(jax.random.uniform(second, (D,), jnp.float32, jnp.log(0.7), jnp.log(1.4)))
    column_scale = jnp.exp(jnp.log(3.0) * column_place) * rough
    pairing = jax.random.permutation(third, N_TP)
    row_block = jnp.arange(MW, dtype=jnp.int32) // (MW // N_TP)
    col_block = jnp.arange(D, dtype=jnp.int32) // (D // N_TP)
    spiked = pairing[row_block][:, None] == col_block[None, :]
    boost = jnp.where(spiked, 4.0, 1.0)
    values = base * boost * column_scale[None, :] / jnp.sqrt(16.0 * MW)
    return values.astype(jnp.bfloat16)


def levels(key, extent, shards, smallest, high):
    factor_of = 1.0
    for axis_at, blocks in shards:
        steps = jax.random.uniform(jax.random.fold_in(jax.random.fold_in(key, 6), axis_at), (blocks,), jnp.float32, smallest / len(shards), high / len(shards))
        factor_of = factor_of * jnp.repeat(jnp.exp(steps), extent[axis_at] // blocks).reshape((-1,) + (1,) * (len(extent) - 1 - axis_at))
    return factor_of


def length_profile(number_of, total, limit, slope):
    portions = [(1 << 20) // math.isqrt(standing ** slope) + 1 for standing in range(2, number_of + 1)]
    spare, holding = total - limit - (number_of - 1), [1] * (number_of - 1)
    while spare > 0:
        free = [i for i in range(number_of - 1) if holding[i] < limit]
        pool, remaining = sum([portions[i] for i in free]), spare
        for i in free:
            more = min(limit - holding[i], max(1, remaining * portions[i] // pool), spare)
            holding[i] = holding[i] + more
            spare = spare - more
    return np.array([limit] + holding)


def uneven(stream_key, number_of, total, limit, lean):
    if number_of == 2:
        one = jax.random.randint(stream_key, (), max(1, total - limit), min(limit, total - 1) + 1)
        return jnp.stack([one, total - one])
    tallies = jnp.asarray(length_profile(number_of, total, limit, lean), jnp.int32)
    twos = (number_of - 1) // 2
    source_of, receiver = tallies[1:1 + 2 * twos:2], tallies[2:2 + 2 * twos:2]
    slack = jnp.minimum(source_of - 1, limit - receiver)
    moved = jax.random.randint(jax.random.fold_in(stream_key, 1), (twos,), 0, 1 << 20) % (slack + 1)
    tallies = tallies.at[1:1 + 2 * twos:2].set(source_of - moved).at[2:2 + 2 * twos:2].set(receiver + moved)
    return tallies[jax.random.permutation(jax.random.fold_in(stream_key, 2), number_of)]


def bell_draw(rng, dims, scale, reach, pieces=(), kind=jnp.bfloat16):
    factor_of = levels(rng, dims, pieces, -0.22, 0.18) if pieces else 1.0
    entries = jax.random.normal(rng, dims, jnp.float32) * scale * factor_of
    return jnp.minimum(jnp.maximum(entries, -reach), reach).astype(kind)


def setup_inputs(seed: int = 0) -> dict:
    streams_of = jax.random.split(jax.random.key(seed), 13)
    return {
        "vit_input": bell_draw(streams_of[0], (PATCHES, VW), 1.0, 6.0, ((0, 128),)),
        "image_lengths": jax.vmap(lambda own: uneven(own, IMG_GROUP, GROUP_TOK, GROUP_TOK * 3 // 4, 2))(jax.random.split(streams_of[1], GROUPS)).reshape((GROUPS, IMG_GROUP)).astype(jnp.int32),
        "positions": jax.random.permutation(streams_of[2], TOKENS).astype(jnp.int32),
        "vit_ln_gain": jnp.clip(1.0 + 0.15 * jax.random.normal(streams_of[3], (VW,), jnp.float32), 0.25, 1.75),
        "w_qkv": bell_draw(streams_of[4], (VW, 3, VW), VW ** -0.5, 0.15625, ((2, 16),)),
        "w_proj": bell_draw(streams_of[5], (VW, VW), VW ** -0.5, 0.15625, ((0, 16),)),
        "merger_ln_gain": jnp.clip(1.0 + 0.15 * jax.random.normal(streams_of[6], (VW,), jnp.float32), 0.25, 1.75),
        "merger_w1": bell_draw(streams_of[7], (MW, MW), MW ** -0.5, 0.078125, ((1, 16),)),
        "merger_w2": draw_merger_w2(jax.random.fold_in(streams_of[12], 71), 0),
        "norm_gain": jnp.clip(1.0 + 0.15 * jax.random.normal(streams_of[9], (D,), jnp.float32), 0.25, 1.75),
        "gate_up_weight": bell_draw(streams_of[10], (D, 2, FF), D ** -0.5, 0.0625, ((0, 8), (2, 16))),
        "down_weight": bell_draw(streams_of[11], (FF, D), (FF // 16) ** -0.5, 0.125, ((0, 16), (1, 8))),
    }


def layer_norm(values, gain):
    mean = lax.optimization_barrier(jnp.mean(values, axis=-1, keepdims=True))
    centered = values - mean
    variance = lax.optimization_barrier(jnp.mean(centered * centered, axis=-1, keepdims=True))
    return centered * lax.rsqrt(variance + 1e-06) * gain

def image_ids(lengths, count):
    image_ends = jnp.cumsum(lengths.astype(jnp.int32)) * 4
    patch_index = jnp.arange(count, dtype=jnp.int32)
    return lax.optimization_barrier(jnp.sum((patch_index[:, None] >= image_ends[None, :]).astype(jnp.int32), axis=1))

def wire_round(values):
    return lax.optimization_barrier(values.astype(jnp.bfloat16)).astype(jnp.float32)

def attend(query, keys, values, image_index):
    scores = jnp.einsum('qhe,khe->hqk', query.astype(jnp.float32), keys.astype(jnp.float32)) * HD ** (-0.5)
    same_image = image_index[:, None] == image_index[None, :]
    scores = jnp.where(same_image[None], scores, -1e+30)
    top = lax.optimization_barrier(jnp.max(scores, axis=-1, keepdims=True))
    expo = jnp.exp(scores - top)
    weights = (expo / lax.optimization_barrier(jnp.sum(expo, axis=-1, keepdims=True))).astype(jnp.bfloat16)
    output = jnp.einsum('hqk,khe->qhe', weights.astype(jnp.float32), values.astype(jnp.float32))
    return output.astype(jnp.bfloat16)

def slot_sources(positions):
    count = positions.shape[0]
    return jnp.zeros((count,), jnp.int32).at[positions.astype(jnp.int32)].set(jnp.arange(count, dtype=jnp.int32))

def reference(vit_input, image_lengths, positions, vit_ln_gain, w_qkv, w_proj, merger_ln_gain, merger_w1, merger_w2, norm_gain, gate_up_weight, down_weight):
    group_patches = PATCHES // N_SEQ
    normed_patches = layer_norm(vit_input.astype(jnp.float32), vit_ln_gain).astype(jnp.bfloat16)
    projected = jnp.dot(normed_patches, w_qkv.reshape(VW, 3 * VW), preferred_element_type=jnp.float32).astype(jnp.bfloat16)
    projected = projected.reshape(N_SEQ, group_patches, 3, HEADS, HD)

    def per_group(pair):
        block, lengths = pair
        image_index = image_ids(lengths, group_patches)
        return attend(block[:, 0], block[:, 1], block[:, 2], image_index)
    attended = lax.map(per_group, (projected, image_lengths)).reshape(PATCHES, VW)
    head_cols = VW // N_TP
    attn_sum = jnp.zeros((PATCHES, VW), jnp.float32)
    for block_index in range(N_TP):
        lower = block_index * head_cols
        attn_sum = attn_sum + wire_round(jnp.dot(attended[:, lower:lower + head_cols], w_proj[lower:lower + head_cols], preferred_element_type=jnp.float32))
    vit_out = vit_input.astype(jnp.float32) + attn_sum
    merged_in = layer_norm(vit_out, merger_ln_gain).astype(jnp.bfloat16).reshape(TOKENS, MW)
    expanded = jax.nn.gelu(jnp.dot(merged_in, merger_w1, preferred_element_type=jnp.float32), approximate=False).astype(jnp.bfloat16)
    merge_cols = MW // N_TP
    vis_sum = jnp.zeros((TOKENS, D), jnp.float32)
    for block_index in range(N_TP):
        lower = block_index * merge_cols
        vis_sum = vis_sum + wire_round(jnp.dot(expanded[:, lower:lower + merge_cols], merger_w2[lower:lower + merge_cols], preferred_element_type=jnp.float32))
    vis = vis_sum.astype(jnp.bfloat16)
    seq_tokens = jnp.take(vis, slot_sources(positions), axis=0)
    token_values = seq_tokens.astype(jnp.float32)
    row_squares = lax.optimization_barrier(jnp.sum(token_values * token_values, axis=1))
    inverse_rms = lax.rsqrt(row_squares / D + 1e-06)
    normed = (token_values * inverse_rms[:, None] * norm_gain).astype(jnp.bfloat16)
    slice_width = D // N_SEQ
    gate_up = jnp.zeros((TOKENS, 2 * FF), jnp.float32)
    for block_index in range(N_SEQ):
        lower = block_index * slice_width
        weight_block = gate_up_weight[lower:lower + slice_width].reshape(slice_width, 2 * FF)
        gate_up = gate_up + wire_round(jnp.dot(normed[:, lower:lower + slice_width], weight_block, preferred_element_type=jnp.float32))
    hidden = (jax.nn.silu(gate_up[:, :FF]) * gate_up[:, FF:]).astype(jnp.bfloat16)
    hidden_cols = FF // N_TP
    down_sum = jnp.zeros((TOKENS, D), jnp.float32)
    for block_index in range(N_TP):
        lower = block_index * hidden_cols
        down_sum = down_sum + wire_round(jnp.dot(hidden[:, lower:lower + hidden_cols], down_weight[lower:lower + hidden_cols], preferred_element_type=jnp.float32))
    return (token_values + down_sum).astype(jnp.bfloat16)
```

```python
import functools
import jax
import jax.numpy as jnp
from jax import lax
from jax.experimental import pallas as pl
from jax.experimental.pallas import tpu as pltpu
from jax.sharding import Mesh
from jax.sharding import PartitionSpec as P

MESH_ID = pl.DeviceIdType.MESH
AXES = ("tp_0", "tp_1")


def ring(axis, step):
    return {axis: lax.rem(lax.axis_index(axis) + step, 4)}


def remote(src, dst, send, recv, target):
    return pltpu.make_async_remote_copy(
        src_ref=src, dst_ref=dst, send_sem=send, recv_sem=recv, device_id=target, device_id_type=MESH_ID
    )


def greet(targets):
    barrier = pltpu.get_barrier_semaphore()
    for target in targets:
        pl.semaphore_signal(barrier, inc=1, device_id=target, device_id_type=MESH_ID)
    pl.semaphore_wait(barrier, len(targets))


def plane_neighbours():
    return [ring(axis, step) for axis in AXES for step in (1, 3)]


def gather_plane(own, slot, half_cut, quarter_cut, send, recv, ready=None):
    here = [lax.axis_index(axis) for axis in AXES]
    sent = []

    def place(half, first, second):
        offsets = (first, second) if half == 0 else (second, first)
        spots = [lax.rem(at + off, 4) for at, off in zip(here, offsets)]
        return slot(spots[0] * 4 + spots[1])

    def source(half, first, second):
        return own if (first, second) == (0, 0) else place(half, first, second)

    def start(half, phase, kind, axis, step, first, second, cut):
        at = half * 20 + phase * 4 + kind
        copy = remote(
            cut(source(half, first, second)), cut(place(half, first, second)), send.at[at], recv.at[at], ring(axis, step)
        )
        copy.start()
        sent.append(copy)

    def landed(half, phase, kind, axis, first, second, cut):
        at = half * 20 + phase * 4 + kind
        target = cut(place(half, first, second))
        remote(target, target, send.at[at], recv.at[at], ring(axis, 1)).wait_recv()

    def axes(half):
        return (AXES[0], AXES[1]) if half == 0 else (AXES[1], AXES[0])

    def cuts(half):
        return (
            lambda ref: half_cut(ref, half),
            lambda ref: quarter_cut(ref, 2 * half),
            lambda ref: quarter_cut(ref, 2 * half + 1),
        )

    def spread(half, phase, first):
        whole, _, _ = cuts(half)
        axis = axes(half)[1]
        start(half, phase, 0, axis, 1, first, 0, whole)
        start(half, phase, 1, axis, 3, first, 0, whole)

    def relay(half, phase, first):
        whole, low, high = cuts(half)
        axis = axes(half)[1]
        landed(half, phase, 0, axis, first, 3, whole)
        start(half, phase, 2, axis, 1, first, 3, low)
        landed(half, phase, 1, axis, first, 1, whole)
        start(half, phase, 3, axis, 3, first, 1, high)

    def finish(half, phase, first):
        whole, low, high = cuts(half)
        axis = axes(half)[1]
        landed(half, phase, 2, axis, first, 2, low)
        landed(half, phase, 3, axis, first, 2, high)

    for half in (0, 1):
        whole, _, _ = cuts(half)
        start(half, 0, 0, axes(half)[0], 1, 0, 0, whole)
        start(half, 0, 1, axes(half)[0], 3, 0, 0, whole)
    for half in (0, 1):
        spread(half, 1, 0)
    for half in (0, 1):
        whole, low, high = cuts(half)
        axis = axes(half)[0]
        landed(half, 0, 0, axis, 3, 0, whole)
        start(half, 0, 2, axis, 1, 3, 0, low)
        spread(half, 2, 3)
        landed(half, 0, 1, axis, 1, 0, whole)
        start(half, 0, 3, axis, 3, 1, 0, high)
        spread(half, 3, 1)
    for half in (0, 1):
        relay(half, 1, 0)
    for half in (0, 1):
        whole, low, high = cuts(half)
        axis = axes(half)[0]
        landed(half, 0, 2, axis, 2, 0, low)
        landed(half, 0, 3, axis, 2, 0, high)
        spread(half, 4, 2)
    for phase, first in ((2, 3), (3, 1), (4, 2)):
        for half in (0, 1):
            relay(half, phase, first)
    for phase, first in ((1, 0), (2, 3), (3, 1), (4, 2)):
        for half in (0, 1):
            finish(half, phase, first)
    for copy in sent:
        copy.wait_send()


def reduce_plane(term, quarter_cut, got, made, sums, send, recv, emit):
    here = [lax.axis_index(axis) for axis in AXES]
    sent = []

    def axes(half):
        return (AXES[1], AXES[0]) if half == 0 else (AXES[0], AXES[1])

    def part(half, first, second, which):
        offsets = (first, second) if half == 0 else (second, first)
        spots = [lax.rem(at + off, 4) for at, off in zip(here, offsets)]
        return quarter_cut(term(spots[0] * 4 + spots[1]), 2 * half + which)

    def phase_source(half, phase):
        if phase < 4:
            return lambda offset, which: part(half, phase, offset, which)
        return lambda offset, which: sums.at[half * 8 + offset * 2 + which]

    def slot(half, phase, kind):
        return half * 30 + phase * 6 + kind

    def start(half, phase, kind, src, step):
        axis = axes(half)[0 if phase < 4 else 1]
        at = slot(half, phase, kind)
        copy = remote(src, got.at[at], send.at[at], recv.at[at], ring(axis, step))
        copy.start()
        sent.append(copy)

    def landed(half, phase, kind):
        at = slot(half, phase, kind)
        axis = axes(half)[0 if phase < 4 else 1]
        remote(got.at[at], got.at[at], send.at[at], recv.at[at], ring(axis, 1)).wait_recv()
        return got[at].astype(jnp.float32)

    def raw(half, phase):
        own = phase_source(half, phase)
        start(half, phase, 0, own(2, 0), 1)
        start(half, phase, 3, own(2, 1), 3)
        start(half, phase, 1, own(1, 1), 1)
        start(half, phase, 4, own(3, 0), 3)

    def summed(half, phase):
        own = phase_source(half, phase)
        for kind, offset, which, step in ((0, 1, 0, 1), (3, 3, 1, 3)):
            at = half * 10 + phase * 2 + which
            made[at] = (own(offset, which)[...].astype(jnp.float32) + landed(half, phase, kind)).astype(made.dtype)
            start(half, phase, kind + 2, made.at[at], step)

    def total(half, phase):
        own = phase_source(half, phase)
        return [
            own(0, which)[...].astype(jnp.float32) + landed(half, phase, near) + landed(half, phase, far)
            for which, near, far in ((0, 4, 2), (1, 1, 5))
        ]

    def settle(half, phase):
        for which, value in enumerate(total(half, phase)):
            sums[half * 8 + phase * 2 + which] = value.astype(sums.dtype)

    order = (2, 1, 3, 0)
    both = (0, 1)
    for half in both:
        raw(half, order[0])
    for half in both:
        raw(half, order[1])
    for at, phase in enumerate(order):
        for half in both:
            summed(half, phase)
        if at + 2 < 4:
            for half in both:
                raw(half, order[at + 2])
        if at >= 1:
            for half in both:
                settle(half, order[at - 1])
                if order[at - 1] == 2:
                    own = phase_source(half, 4)
                    start(half, 4, 0, own(2, 0), 1)
                    start(half, 4, 3, own(2, 1), 3)
                if order[at - 1] == 1:
                    start(half, 4, 1, phase_source(half, 4)(1, 1), 1)
                if order[at - 1] == 3:
                    start(half, 4, 4, phase_source(half, 4)(3, 0), 3)
    for half in both:
        summed(half, 4)
    for half in both:
        settle(half, 0)
    for half in both:
        for which, value in enumerate(total(half, 4)):
            emit(2 * half + which, value)
    for copy in sent:
        copy.wait_send()


def cut_rows(ref, begin, size):
    return ref.at[pl.ds(begin, size)]


def plane_gather(block, collective_id, by_rows):
    rows, cols = block.shape

    def cutter(share):
        def cut(ref, at):
            if by_rows:
                return ref.at[pl.ds(at * (rows // share), rows // share), :]
            return ref.at[:, pl.ds(at * (cols // share), cols // share)]
        return cut

    def kernel(own, out, send, recv):
        greet(plane_neighbours())
        me = lax.axis_index("tp_0") * 4 + lax.axis_index("tp_1")
        out[me] = own[...]
        gather_plane(own, lambda t: out.at[t], cutter(2), cutter(4), send, recv)

    return pl.pallas_call(
        kernel,
        out_shape=jax.ShapeDtypeStruct((16, rows, cols), block.dtype),
        in_specs=[pl.BlockSpec(memory_space=pltpu.VMEM)],
        out_specs=pl.BlockSpec(memory_space=pltpu.VMEM),
        scratch_shapes=[pltpu.SemaphoreType.DMA((40,)), pltpu.SemaphoreType.DMA((40,))],
        compiler_params=pltpu.CompilerParams(collective_id=collective_id, has_side_effects=True),
        name=f"plane_gather_{collective_id}",
    )(block)


def plane_reduce(terms, collective_id, by_rows, out_dtype):
    _, rows, cols = terms.shape
    quarter = (rows // 4, cols) if by_rows else (rows, cols // 4)

    def cut(ref, at):
        if by_rows:
            return ref.at[pl.ds(at * quarter[0], quarter[0]), :]
        return ref.at[:, pl.ds(at * quarter[1], quarter[1])]

    def kernel(terms_ref, out, got, made, sums, send, recv):
        greet(plane_neighbours())

        def emit(at, value):
            cut(out, at)[...] = value.astype(out.dtype)

        reduce_plane(lambda t: terms_ref.at[t], cut, got, made, sums, send, recv, emit)

    return pl.pallas_call(
        kernel,
        out_shape=jax.ShapeDtypeStruct((rows, cols), out_dtype),
        in_specs=[pl.BlockSpec(memory_space=pltpu.VMEM)],
        out_specs=pl.BlockSpec(memory_space=pltpu.VMEM),
        scratch_shapes=[
            pltpu.VMEM((60, *quarter), terms.dtype),
            pltpu.VMEM((20, *quarter), terms.dtype),
            pltpu.VMEM((16, *quarter), terms.dtype),
            pltpu.SemaphoreType.DMA((60,)),
            pltpu.SemaphoreType.DMA((60,)),
        ],
        compiler_params=pltpu.CompilerParams(collective_id=collective_id, has_side_effects=True),
        name=f"plane_reduce_{collective_id}",
    )(terms)

D = 8192
HD = 80
TP = ("tp_0", "tp_1")
SEQ_TP = ("seq", "tp_0", "tp_1")


def from_everyone(x, axis):
    copies = jnp.broadcast_to(x, (lax.axis_size(axis), *x.shape))
    return lax.all_to_all(copies, axis, split_axis=0, concat_axis=0, tiled=True)


def laid_out(tiles, dim):
    shape = list(tiles.shape[1:])
    shape[dim] *= tiles.shape[0]
    return jnp.moveaxis(tiles, 0, dim).reshape(shape)


def gathered_copies(x, axis, dim):
    tiles = from_everyone(x, axis)
    return laid_out(tiles, dim)


def cut_along(x, dim, devices):
    before, after = (x.shape[:dim], x.shape[dim + 1 :])
    return jnp.moveaxis(x.reshape(*before, devices, -1, *after), dim, 0)


def sum_at_owner(x, axis, dim):
    devices = lax.axis_size(axis)
    tiles = lax.all_to_all(cut_along(x, dim, devices), axis, 0, 0, tiled=True)
    return jnp.sum(tiles.astype(jnp.float32), axis=0)


def over_copies(x, axis):
    everything = from_everyone(x, axis)
    return jnp.sum(everything, axis=0)


def sum_by_axis(x, axes, dim):
    if not axes:
        return x
    nearer = lax.psum_scatter(x, axes[0], scatter_dimension=dim, tiled=True)
    return sum_by_axis(nearer, axes[1:], dim)


def layer_norm(values, gain):
    mean = jnp.mean(values, axis=-1, keepdims=True)
    centered = values - mean
    variance = jnp.mean(centered * centered, axis=-1, keepdims=True)
    return centered * lax.rsqrt(variance + 1e-06) * gain


def image_ids(lengths, count):
    image_ends = jnp.cumsum(lengths) * 4
    patch_index = jnp.arange(count, dtype=jnp.int32)
    return jnp.sum((patch_index[:, None] >= image_ends[None, :]).astype(jnp.int32), axis=1)


def attend(query, keys, values, image_index):
    scores = jnp.einsum("qhe,khe->hqk", query, keys, preferred_element_type=jnp.float32) * HD ** (
        -0.5
    )
    same_image = image_index[:, None] == image_index[None, :]
    scores = jnp.where(same_image[None], scores, -1e30)
    top = jnp.max(scores, axis=-1, keepdims=True)
    expo = jnp.exp(scores - top)
    weights = (expo / jnp.sum(expo, axis=-1, keepdims=True)).astype(jnp.bfloat16)
    output = jnp.einsum("hqk,khe->qhe", weights, values, preferred_element_type=jnp.float32)
    return output.astype(jnp.bfloat16)


def slot_sources(positions):
    count = positions.shape[0]
    return jnp.zeros((count,), jnp.int32).at[positions].set(jnp.arange(count, dtype=jnp.int32))


def local(
    vit_input,
    image_lengths,
    positions,
    vit_ln_gain,
    w_qkv,
    w_proj,
    merger_ln_gain,
    merger_w1,
    merger_w2,
    norm_gain,
    gate_up_weight,
    down_weight,
):
    tp_size = lax.axis_size(TP)
    seq_size = lax.axis_size("seq")
    own_patches = vit_input.shape[0]
    patch_width = vit_input.shape[1]
    head_cols = w_qkv.shape[2]
    local_heads = head_cols // HD
    normed_patches = layer_norm(vit_input.astype(jnp.float32), vit_ln_gain).astype(jnp.bfloat16)
    w_qkv_flat = w_qkv.reshape(patch_width, 3 * head_cols)
    projected = jnp.dot(
        plane_gather(normed_patches, 1, True).reshape(-1, patch_width), w_qkv_flat, preferred_element_type=jnp.float32
    ).astype(jnp.bfloat16)
    group_patches = projected.shape[0]
    projected = projected.reshape(group_patches, 3, local_heads, HD)
    image_index = image_ids(image_lengths[0], group_patches)
    attended = attend(projected[:, 0], projected[:, 1], projected[:, 2], image_index).reshape(
        group_patches, head_cols
    )
    picked = attended
    shares = jnp.dot(picked, w_proj, preferred_element_type=jnp.float32).astype(jnp.bfloat16)
    attn_sum = plane_reduce(shares.reshape(tp_size, own_patches, patch_width), 2, True, jnp.float32)
    vit_out = vit_input.astype(jnp.float32) + attn_sum
    own_tokens = own_patches // 4
    merged_in = (
        layer_norm(vit_out, merger_ln_gain)
        .astype(jnp.bfloat16)
        .reshape(own_tokens, 4 * patch_width)
    )
    expanded = jax.nn.gelu(
        jnp.dot(plane_gather(merged_in, 3, False).reshape(-1, 4 * patch_width), merger_w1, preferred_element_type=jnp.float32),
        approximate=False,
    ).astype(jnp.bfloat16)
    picked = expanded
    shares = jnp.dot(picked, merger_w2, preferred_element_type=jnp.float32).astype(jnp.bfloat16)
    vis_rows = plane_reduce(shares.reshape(tp_size, own_tokens, D), 4, False, jnp.bfloat16)
    blocks = lax.all_to_all(vis_rows, "seq", split_axis=1, concat_axis=0, tiled=True)
    gathered = plane_gather(blocks, 5, True)
    col_width = gathered.shape[2]
    all_tokens = (
        gathered.reshape(tp_size, seq_size, own_tokens, col_width)
        .transpose(1, 0, 2, 3)
        .reshape(tp_size * seq_size * own_tokens, col_width)
    )
    seq_rows = all_tokens.shape[0]
    seq_tokens = jnp.take(all_tokens, slot_sources(positions), axis=0)
    token_values = seq_tokens.astype(jnp.float32)
    row_squares = over_copies(jnp.sum(token_values * token_values, axis=1), "seq")
    inverse_rms = lax.rsqrt(row_squares / D + 1e-06)
    normed = (token_values * inverse_rms[:, None] * norm_gain).astype(jnp.bfloat16)
    slice_width = seq_tokens.shape[1]
    hidden_width = gate_up_weight.shape[2]
    weight_flat = gate_up_weight.reshape(slice_width, 2 * hidden_width)
    out_rows = seq_rows // tp_size
    picked = normed
    gate_up = lax.psum_scatter(
        jnp.dot(picked, weight_flat, preferred_element_type=jnp.float32).astype(jnp.bfloat16),
        "seq",
        scatter_dimension=0,
        tiled=True,
    ).astype(jnp.float32)
    hidden = (jax.nn.silu(gate_up[:, :hidden_width]) * gate_up[:, hidden_width:]).astype(
        jnp.bfloat16
    )
    terms = jnp.dot(
        lax.all_gather(hidden, "seq", axis=0, tiled=True),
        down_weight,
        preferred_element_type=jnp.float32,
    )
    down_sum = sum_by_axis(terms.astype(jnp.bfloat16), TP, 0).astype(jnp.float32)
    residual = lax.dynamic_slice_in_dim(token_values, lax.axis_index(TP) * out_rows, out_rows, 0)
    return (residual + down_sum).astype(jnp.bfloat16)


def solution(mesh):
    finer = Mesh(mesh.devices.reshape(mesh.shape["seq"], 4, 4), ("seq", "tp_0", "tp_1"))
    in_specs = (
        P(SEQ_TP, None),
        P("seq", None),
        P(),
        P(),
        P(None, None, TP),
        P(TP, None),
        P(),
        P(None, TP),
        P(TP, None),
        P("seq"),
        P("seq", None, TP),
        P(TP, "seq"),
    )
    out_specs = P(TP, "seq")
    return jax.shard_map(local, mesh=finer, in_specs=in_specs, out_specs=out_specs, check_vma=False)
```

```python
import functools
import jax
import jax.numpy as jnp
from jax import lax
from jax.experimental import pallas as pl
from jax.experimental.pallas import tpu as pltpu
from jax.sharding import Mesh
from jax.sharding import PartitionSpec as P

D = 8192
HD = 80
TP = ("tp_0", "tp_1")
SEQ_TP = ("seq", "tp_0", "tp_1")

MESH_ID = pl.DeviceIdType.MESH
AXES = ("tp_0", "tp_1")


def ring(axis, step):
    return {axis: lax.rem(lax.axis_index(axis) + step, 4)}


def remote(src, dst, send, recv, target):
    return pltpu.make_async_remote_copy(
        src_ref=src, dst_ref=dst, send_sem=send, recv_sem=recv, device_id=target, device_id_type=MESH_ID
    )


def greet(targets):
    barrier = pltpu.get_barrier_semaphore()
    for target in targets:
        pl.semaphore_signal(barrier, inc=1, device_id=target, device_id_type=MESH_ID)
    pl.semaphore_wait(barrier, len(targets))


def plane_neighbours():
    return [ring(axis, step) for axis in AXES for step in (1, 3)]


def gather_plane(own, slot, half_cut, quarter_cut, send, recv, forward=None):
    here = [lax.axis_index(axis) for axis in AXES]
    sent = []

    def index(half, first, second):
        offsets = (first, second) if half == 0 else (second, first)
        spots = [lax.rem(at + off, 4) for at, off in zip(here, offsets)]
        return spots[0] * 4 + spots[1]

    def place(half, first, second):
        return slot(index(half, first, second))

    def source(half, first, second):
        return own if (first, second) == (0, 0) else place(half, first, second)

    def start(half, phase, kind, axis, step, first, second, cut):
        at = half * 20 + phase * 4 + kind
        copy = remote(
            cut(source(half, first, second)), cut(place(half, first, second)), send.at[at], recv.at[at], ring(axis, step)
        )
        copy.start()
        sent.append(copy)

    def landed(half, phase, kind, axis, first, second, cut):
        at = half * 20 + phase * 4 + kind
        target = cut(place(half, first, second))
        remote(target, target, send.at[at], recv.at[at], ring(axis, 1)).wait_recv()
        if forward is not None:
            forward(at, lambda base: cut(base(index(half, first, second))))

    def axes(half):
        return (AXES[0], AXES[1]) if half == 0 else (AXES[1], AXES[0])

    def cuts(half):
        return (
            lambda ref: half_cut(ref, half),
            lambda ref: quarter_cut(ref, 2 * half),
            lambda ref: quarter_cut(ref, 2 * half + 1),
        )

    def spread(half, phase, first):
        whole, _, _ = cuts(half)
        axis = axes(half)[1]
        start(half, phase, 0, axis, 1, first, 0, whole)
        start(half, phase, 1, axis, 3, first, 0, whole)

    def relay(half, phase, first):
        whole, low, high = cuts(half)
        axis = axes(half)[1]
        landed(half, phase, 0, axis, first, 3, whole)
        start(half, phase, 2, axis, 1, first, 3, low)
        landed(half, phase, 1, axis, first, 1, whole)
        start(half, phase, 3, axis, 3, first, 1, high)

    def finish(half, phase, first):
        whole, low, high = cuts(half)
        axis = axes(half)[1]
        landed(half, phase, 2, axis, first, 2, low)
        landed(half, phase, 3, axis, first, 2, high)

    for half in (0, 1):
        whole, _, _ = cuts(half)
        start(half, 0, 0, axes(half)[0], 1, 0, 0, whole)
        start(half, 0, 1, axes(half)[0], 3, 0, 0, whole)
    for half in (0, 1):
        spread(half, 1, 0)
    for half in (0, 1):
        whole, low, high = cuts(half)
        axis = axes(half)[0]
        landed(half, 0, 0, axis, 3, 0, whole)
        start(half, 0, 2, axis, 1, 3, 0, low)
        spread(half, 2, 3)
        landed(half, 0, 1, axis, 1, 0, whole)
        start(half, 0, 3, axis, 3, 1, 0, high)
        spread(half, 3, 1)
    for half in (0, 1):
        relay(half, 1, 0)
    for half in (0, 1):
        whole, low, high = cuts(half)
        axis = axes(half)[0]
        landed(half, 0, 2, axis, 2, 0, low)
        landed(half, 0, 3, axis, 2, 0, high)
        spread(half, 4, 2)
    for phase, first in ((2, 3), (3, 1), (4, 2)):
        for half in (0, 1):
            relay(half, phase, first)
    for phase, first in ((1, 0), (2, 3), (3, 1), (4, 2)):
        for half in (0, 1):
            finish(half, phase, first)
    for copy in sent:
        copy.wait_send()


def reduce_plane(term, got, made, sums, send, recv, emit):
    here = [lax.axis_index(axis) for axis in AXES]
    sent = []

    def axes(half):
        return (AXES[1], AXES[0]) if half == 0 else (AXES[0], AXES[1])

    def part(half, first, second, which):
        offsets = (first, second) if half == 0 else (second, first)
        spots = [lax.rem(at + off, 4) for at, off in zip(here, offsets)]
        return term(spots[0] * 4 + spots[1], 2 * half + which)

    def phase_source(half, phase):
        if phase < 4:
            return lambda offset, which: part(half, phase, offset, which)
        return lambda offset, which: sums.at[half * 8 + offset * 2 + which]

    def slot(half, phase, kind):
        return half * 30 + phase * 6 + kind

    def start(half, phase, kind, src, step):
        axis = axes(half)[0 if phase < 4 else 1]
        at = slot(half, phase, kind)
        copy = remote(src, got.at[at], send.at[at], recv.at[at], ring(axis, step))
        copy.start()
        sent.append(copy)

    def landed(half, phase, kind):
        at = slot(half, phase, kind)
        axis = axes(half)[0 if phase < 4 else 1]
        remote(got.at[at], got.at[at], send.at[at], recv.at[at], ring(axis, 1)).wait_recv()
        return got[at].astype(jnp.float32)

    def raw(half, phase):
        own = phase_source(half, phase)
        start(half, phase, 0, own(2, 0), 1)
        start(half, phase, 3, own(2, 1), 3)
        start(half, phase, 1, own(1, 1), 1)
        start(half, phase, 4, own(3, 0), 3)

    def summed(half, phase):
        own = phase_source(half, phase)
        for kind, offset, which, step in ((0, 1, 0, 1), (3, 3, 1, 3)):
            at = half * 10 + phase * 2 + which
            made[at] = (own(offset, which)[...].astype(jnp.float32) + landed(half, phase, kind)).astype(made.dtype)
            start(half, phase, kind + 2, made.at[at], step)

    def total(half, phase):
        own = phase_source(half, phase)
        return [
            own(0, which)[...].astype(jnp.float32) + landed(half, phase, near) + landed(half, phase, far)
            for which, near, far in ((0, 4, 2), (1, 1, 5))
        ]

    def settle(half, phase):
        for which, value in enumerate(total(half, phase)):
            sums[half * 8 + phase * 2 + which] = value.astype(sums.dtype)

    order = (2, 1, 3, 0)
    both = (0, 1)
    for half in both:
        raw(half, order[0])
    for half in both:
        raw(half, order[1])
    for at, phase in enumerate(order):
        for half in both:
            summed(half, phase)
        if at + 2 < 4:
            for half in both:
                raw(half, order[at + 2])
        if at >= 1:
            for half in both:
                settle(half, order[at - 1])
                if order[at - 1] == 2:
                    own = phase_source(half, 4)
                    start(half, 4, 0, own(2, 0), 1)
                    start(half, 4, 3, own(2, 1), 3)
                if order[at - 1] == 1:
                    start(half, 4, 1, phase_source(half, 4)(1, 1), 1)
                if order[at - 1] == 3:
                    start(half, 4, 4, phase_source(half, 4)(3, 0), 3)
    for half in both:
        summed(half, 4)
    for half in both:
        settle(half, 0)
    for half in both:
        for which, value in enumerate(total(half, 4)):
            emit(2 * half + which, value)
    for copy in sent:
        copy.wait_send()


def cut_rows(ref, begin, size):
    return ref.at[pl.ds(begin, size)]


def plane_gather(block, collective_id, by_rows):
    rows, cols = block.shape

    def cutter(share):
        def cut(ref, at):
            if by_rows:
                return ref.at[pl.ds(at * (rows // share), rows // share), :]
            return ref.at[:, pl.ds(at * (cols // share), cols // share)]
        return cut

    def kernel(own, out, send, recv):
        greet(plane_neighbours())
        me = lax.axis_index("tp_0") * 4 + lax.axis_index("tp_1")
        out[me] = own[...]
        gather_plane(own, lambda t: out.at[t], cutter(2), cutter(4), send, recv)

    return pl.pallas_call(
        kernel,
        out_shape=jax.ShapeDtypeStruct((16, rows, cols), block.dtype),
        in_specs=[pl.BlockSpec(memory_space=pltpu.VMEM)],
        out_specs=pl.BlockSpec(memory_space=pltpu.VMEM),
        scratch_shapes=[pltpu.SemaphoreType.DMA((40,)), pltpu.SemaphoreType.DMA((40,))],
        compiler_params=pltpu.CompilerParams(collective_id=collective_id, has_side_effects=True),
        name=f"plane_gather_{collective_id}",
    )(block)


def plane_reduce(terms, collective_id, by_rows, out_dtype):
    _, rows, cols = terms.shape
    quarter = (rows // 4, cols) if by_rows else (rows, cols // 4)

    def cut(ref, at):
        if by_rows:
            return ref.at[pl.ds(at * quarter[0], quarter[0]), :]
        return ref.at[:, pl.ds(at * quarter[1], quarter[1])]

    def kernel(terms_ref, out, got, made, sums, send, recv):
        greet(plane_neighbours())

        def emit(at, value):
            cut(out, at)[...] = value.astype(out.dtype)

        reduce_plane(lambda t, at: cut(terms_ref.at[t], at), got, made, sums, send, recv, emit)

    return pl.pallas_call(
        kernel,
        out_shape=jax.ShapeDtypeStruct((rows, cols), out_dtype),
        in_specs=[pl.BlockSpec(memory_space=pltpu.VMEM)],
        out_specs=pl.BlockSpec(memory_space=pltpu.VMEM),
        scratch_shapes=[
            pltpu.VMEM((60, *quarter), terms.dtype),
            pltpu.VMEM((20, *quarter), terms.dtype),
            pltpu.VMEM((16, *quarter), terms.dtype),
            pltpu.SemaphoreType.DMA((60,)),
            pltpu.SemaphoreType.DMA((60,)),
        ],
        compiler_params=pltpu.CompilerParams(collective_id=collective_id, has_side_effects=True),
        name=f"plane_reduce_{collective_id}",
    )(terms)
WIDE = 2176
PADDED = 1920


def along_x(step):
    seq = lax.axis_index("seq")
    return {"seq": lax.rem(seq + 2 * step, 8)}


def partner():
    seq = lax.axis_index("seq")
    return {"seq": seq + 1 - 2 * lax.rem(seq, 2)}


def token_kernel(terms_ref, out, got, made, sums, vis, parcels, block, send, recv, xsend, xrecv, gsend, grecv, dsend, drecv):
    greet(plane_neighbours() + [along_x(step) for step in (1, 2, 3)] + [partner()])
    seq = lax.axis_index("seq")
    x, core = seq // 2, lax.rem(seq, 2)
    me = lax.axis_index("tp_0") * 4 + lax.axis_index("tp_1")

    def emit(at, value):
        parcels[at, :, :2048] = value.astype(jnp.bfloat16)

    reduce_plane(lambda t, at: terms_ref.at[t, :, pl.ds(at * 2048, 2048)], got, made, sums, send, recv, emit)
    squares = jnp.zeros((16, 1), jnp.float32)
    for at in range(4):
        values = parcels[at, :, :2048].astype(jnp.float32)
        squares = squares + jnp.sum(values * values, axis=1, keepdims=True)
    high = squares.astype(jnp.bfloat16).astype(jnp.float32)
    low = squares - high
    lane = lax.broadcasted_iota(jnp.int32, (16, 128), 1)
    tail = jnp.where(lane == 0, high, jnp.where(lane == 1, low, 0.0)).astype(jnp.bfloat16)
    for at in range(4):
        parcels[at, :, 2048:] = tail
    mine = pl.ds(pl.multiple_of(x * 16, 16), 16)
    sent = []
    for step in (2, 1, 3):
        copy = remote(
            parcels.at[lax.rem(x + step, 4)], block.at[mine, :], xsend.at[step], xrecv.at[step], along_x(step)
        )
        copy.start()
        sent.append(copy)
    block[mine, :] = parcels[x]
    for step in (1, 3, 2):
        rows = pl.ds(pl.multiple_of(lax.rem(x + 4 - step, 4) * 16, 16), 16)
        landing = block.at[rows, :]
        remote(landing, landing, xsend.at[step], xrecv.at[step], along_x(step)).wait_recv()
    for copy in sent:
        copy.wait_send()
    forwarded = []
    expected = []

    def forward(at, view):
        piece = view(lambda t: out.at[core, t])
        copy = remote(piece, piece, dsend.at[at], drecv.at[at], partner())
        copy.start()
        forwarded.append(copy)
        other = view(lambda t: out.at[1 - core, t])
        expected.append(remote(other, other, dsend.at[at], drecv.at[at], partner()))

    own_copy = remote(block, out.at[core, me], dsend.at[40], drecv.at[40], partner())
    own_copy.start()
    out[core, me] = block[...]
    gather_plane(
        block,
        lambda t: out.at[core, t],
        lambda ref, half: ref.at[pl.ds(half * 32, 32), :],
        lambda ref, at: ref.at[pl.ds(at * 16, 16), :],
        gsend,
        grecv,
        forward,
    )
    other = out.at[1 - core, me]
    expected.append(remote(other, other, dsend.at[40], drecv.at[40], partner()))
    own_copy.wait_send()
    for copy in forwarded:
        copy.wait_send()
    for copy in expected:
        copy.wait_recv()


def all_tokens_of(terms, collective_id):
    return pl.pallas_call(
        token_kernel,
        out_shape=jax.ShapeDtypeStruct((2, 16, 64, WIDE), jnp.bfloat16),
        in_specs=[pl.BlockSpec(memory_space=pltpu.VMEM)],
        out_specs=pl.BlockSpec(memory_space=pltpu.VMEM),
        scratch_shapes=[
            pltpu.VMEM((60, 16, 2048), jnp.bfloat16),
            pltpu.VMEM((20, 16, 2048), jnp.bfloat16),
            pltpu.VMEM((16, 16, 2048), jnp.bfloat16),
            pltpu.VMEM((8, 128), jnp.float32),
            pltpu.VMEM((4, 16, WIDE), jnp.bfloat16),
            pltpu.VMEM((64, WIDE), jnp.bfloat16),
            pltpu.SemaphoreType.DMA((60,)),
            pltpu.SemaphoreType.DMA((60,)),
            pltpu.SemaphoreType.DMA((4,)),
            pltpu.SemaphoreType.DMA((4,)),
            pltpu.SemaphoreType.DMA((40,)),
            pltpu.SemaphoreType.DMA((40,)),
            pltpu.SemaphoreType.DMA((41,)),
            pltpu.SemaphoreType.DMA((41,)),
        ],
        compiler_params=pltpu.CompilerParams(
            collective_id=collective_id, has_side_effects=True, vmem_limit_bytes=48 * 1024 * 1024
        ),
        name="all_tokens",
    )(terms)


def feed_forward_kernel(
    tokens, gain, w_own, w_other, d_own, d_other, out,
    weights, downs, rows, parts, came, hidden, products, got, made, sums, fin,
    wsem, osem, psend, precv, hsend, hrecv, send, recv, fsend, frecv,
):
    seq = lax.axis_index("seq")
    x, core = seq // 2, lax.rem(seq, 2)
    me = lax.axis_index("tp_0") * 4 + lax.axis_index("tp_1")
    real = w_own.shape[1]
    weights[:, pl.ds(1840, 80), :] = jnp.zeros((2, 80, 2048), jnp.bfloat16)
    downs[pl.ds(1840, 80), :] = jnp.zeros((80, 2048), jnp.bfloat16)
    sides = ((w_own, d_own, core), (w_other, d_other, 1 - core))

    def weight_copies(n):
        size = 256 if n < 7 else real - 1792
        return [
            pltpu.make_async_copy(
                w.at[:, pl.ds(n * 256, size), :],
                weights.at[:, pl.ds(n * 256, size), pl.ds(pl.multiple_of(at * 1024, 1024), 1024)],
                wsem.at[n, side],
            )
            for side, (w, _, at) in enumerate(sides)
        ]

    def down_copies():
        return [
            pltpu.make_async_copy(
                d, downs.at[pl.ds(0, real), pl.ds(pl.multiple_of(at * 1024, 1024), 1024)], osem.at[side]
            )
            for side, (_, d, at) in enumerate(sides)
        ]

    for n in range(8):
        for copy in weight_copies(n):
            copy.start()
    for copy in down_copies():
        copy.start()

    def owner(step):
        return lax.rem(x + step, 4)

    def multiply(step, first=False):
        at = owner(step)
        square = tokens[at, :, 2048:2049].astype(jnp.float32) + tokens[at, :, 2049:2050].astype(jnp.float32)
        inverse = lax.rsqrt(square / D + 1e-06)
        rows[...] = (tokens[at, :, :2048].astype(jnp.float32) * inverse * gain[...]).astype(jnp.bfloat16)

        def piece(begin, size):
            for half in range(2):
                value = lax.dot_general(
                    rows[...], weights[half, pl.ds(begin, size), :], (((1,), (1,)), ((), ())),
                    preferred_element_type=jnp.float32,
                )
                parts[step, half, :, pl.ds(begin, size)] = value.astype(jnp.bfloat16)

        if first:
            for n in range(8):
                for copy in weight_copies(n):
                    copy.wait()
                piece(n * 256, 256 if n < 7 else 128)
        else:
            @pl.loop(0, 7)
            def _(n):
                piece(pl.multiple_of(n * 256, 256), 256)

            piece(1792, 128)

    def cut(ref, sub):
        return ref.at[:, pl.ds(sub * 64, 64), :]

    sent = []

    def pass_part(kind, index, src, step):
        at = kind * 2 + index
        copy = remote(src, came.at[at], psend.at[at], precv.at[at], along_x(step))
        copy.start()
        sent.append(copy)

    def part_landed(kind, index):
        at = kind * 2 + index
        remote(came.at[at], came.at[at], psend.at[at], precv.at[at], along_x(1)).wait_recv()
        return came.at[at]

    multiply(2, True)
    greet(plane_neighbours() + [along_x(step) for step in (1, 3)] + [partner()])
    for index in range(2):
        pass_part(0, index, cut(parts.at[2], index), 1)
        pass_part(3, index, cut(parts.at[2], 2 + index), 3)
    multiply(1)
    for index in range(2):
        pass_part(1, index, cut(parts.at[1], 2 + index), 1)
    multiply(3)
    for index in range(2):
        pass_part(4, index, cut(parts.at[3], index), 3)
    for index in range(2):
        for kind, step, sub, way in ((0, 1, index, 1), (3, 3, 2 + index, 3)):
            arrived = part_landed(kind, index)
            target = cut(parts.at[step], sub)
            target[...] = (target[...].astype(jnp.float32) + arrived[...].astype(jnp.float32)).astype(jnp.bfloat16)
            pass_part(kind + 2, index, target, way)
    multiply(0)

    def hidden_piece(step, sub):
        return hidden.at[owner(step), pl.ds(sub * 64, 64), :]

    def pass_hidden(at, piece, step):
        copy = remote(piece, piece, hsend.at[at], hrecv.at[at], along_x(step))
        copy.start()
        sent.append(copy)

    def hidden_landed(at, piece):
        remote(piece, piece, hsend.at[at], hrecv.at[at], along_x(1)).wait_recv()

    for index in range(2):
        for sub, near, far in ((index, 4, 2), (2 + index, 1, 5)):
            one = part_landed(near, index)
            two = part_landed(far, index)
            own = cut(parts.at[0], sub)
            gate, up = [
                own[half].astype(jnp.float32) + one[half].astype(jnp.float32) + two[half].astype(jnp.float32)
                for half in range(2)
            ]
            piece = hidden_piece(0, sub)
            piece[...] = (gate / (1.0 + jnp.exp(-gate)) * up).astype(jnp.bfloat16)
            pass_hidden(sub, piece, 1)
            pass_hidden(4 + sub, piece, 3)
    for copy in down_copies():
        copy.wait()

    def project(step):
        at = owner(step)

        @pl.loop(0, 8)
        def _(n):
            begin = pl.multiple_of(n * 256, 256)
            value = jnp.dot(hidden[at], downs[:, pl.ds(begin, 256)], preferred_element_type=jnp.float32)
            products[at, :, pl.ds(begin, 256)] = value.astype(jnp.bfloat16)

    def relay(index):
        hidden_landed(index, hidden_piece(3, index))
        pass_hidden(8 + index, hidden_piece(3, index), 1)
        hidden_landed(4 + 2 + index, hidden_piece(1, 2 + index))
        pass_hidden(10 + index, hidden_piece(1, 2 + index), 3)

    project(0)
    relay(0)
    relay(1)
    for index in range(2):
        hidden_landed(2 + index, hidden_piece(3, 2 + index))
    project(3)
    for index in range(2):
        hidden_landed(4 + index, hidden_piece(1, index))
    project(1)
    for index in range(2):
        hidden_landed(8 + index, hidden_piece(2, index))
        hidden_landed(10 + index, hidden_piece(2, 2 + index))
    project(2)

    turns = (0, 3, 1, 2)
    strip = pl.ds(pl.multiple_of(me * 16, 16), 16)

    def term(t, at):
        return products.at[owner(turns[at]), pl.ds(pl.multiple_of(t * 16, 16), 16), :]

    def emit(at, value):
        q = owner(turns[at])
        total = (value + tokens[q, strip, :2048].astype(jnp.float32)).astype(jnp.bfloat16)
        target = pl.ds(pl.multiple_of(q * 16, 16), 16)
        fin[0, target, :] = total[:, :1024]
        fin[1, target, :] = total[:, 1024:]

    reduce_plane(term, got, made, sums, send, recv, emit)
    mine = pl.ds(pl.multiple_of(core * 64, 64), 64)
    theirs = pl.ds(pl.multiple_of((1 - core) * 64, 64), 64)
    swap = remote(fin.at[1 - core], out.at[mine, :], fsend, frecv, partner())
    swap.start()
    out[mine, :] = fin[core]
    swap.wait_send()
    landing = out.at[theirs, :]
    remote(landing, landing, fsend, frecv, partner()).wait_recv()
    for copy in sent:
        copy.wait_send()


def feed_forward(tokens, gain, w_own, w_other, d_own, d_other, collective_id):
    anywhere = pl.BlockSpec(memory_space=pl.ANY)
    vmem = pl.BlockSpec(memory_space=pltpu.VMEM)
    dma = pltpu.SemaphoreType.DMA
    bf16 = jnp.bfloat16
    return pl.pallas_call(
        feed_forward_kernel,
        out_shape=jax.ShapeDtypeStruct((128, 1024), bf16),
        in_specs=[vmem, vmem, anywhere, anywhere, anywhere, anywhere],
        out_specs=vmem,
        scratch_shapes=[
            pltpu.VMEM((2, PADDED, 2048), bf16),
            pltpu.VMEM((PADDED, 2048), bf16),
            pltpu.VMEM((256, 2048), bf16),
            pltpu.VMEM((4, 2, 256, PADDED), bf16),
            pltpu.VMEM((12, 2, 64, PADDED), bf16),
            pltpu.VMEM((4, 256, PADDED), bf16),
            pltpu.VMEM((4, 256, 2048), bf16),
            pltpu.VMEM((60, 16, 2048), bf16),
            pltpu.VMEM((20, 16, 2048), bf16),
            pltpu.VMEM((16, 16, 2048), bf16),
            pltpu.VMEM((2, 64, 1024), bf16),
            dma((8, 2)),
            dma((2,)),
            dma((12,)),
            dma((12,)),
            dma((12,)),
            dma((12,)),
            dma((60,)),
            dma((60,)),
            dma,
            dma,
        ],
        compiler_params=pltpu.CompilerParams(
            collective_id=collective_id, has_side_effects=True, vmem_limit_bytes=67043328
        ),
        name="feed_forward",
    )(tokens, gain, w_own, w_other, d_own, d_other)


def layer_norm(values, gain):
    mean = jnp.mean(values, axis=-1, keepdims=True)
    centered = values - mean
    variance = jnp.mean(centered * centered, axis=-1, keepdims=True)
    return centered * lax.rsqrt(variance + 1e-06) * gain


def image_ids(lengths, count):
    image_ends = jnp.cumsum(lengths) * 4
    patch_index = jnp.arange(count, dtype=jnp.int32)
    return jnp.sum((patch_index[:, None] >= image_ends[None, :]).astype(jnp.int32), axis=1)


def attend(query, keys, values, image_index):
    scores = jnp.einsum("qhe,khe->hqk", query, keys, preferred_element_type=jnp.float32) * HD ** (
        -0.5
    )
    same_image = image_index[:, None] == image_index[None, :]
    scores = jnp.where(same_image[None], scores, -1e30)
    top = jnp.max(scores, axis=-1, keepdims=True)
    expo = jnp.exp(scores - top)
    weights = (expo / jnp.sum(expo, axis=-1, keepdims=True)).astype(jnp.bfloat16)
    output = jnp.einsum("hqk,khe->qhe", weights, values, preferred_element_type=jnp.float32)
    return output.astype(jnp.bfloat16)


def sources(positions, core):
    row = jnp.arange(1024, dtype=jnp.int32)
    slot = (row // 16 % 16) * 128 + core * 64 + (row // 256) * 16 + row % 16
    index = jnp.arange(positions.shape[0], dtype=jnp.int32)
    found = jnp.sum(jnp.where(positions[None, :] == slot[:, None], index[None, :], 0), axis=1)
    group, within = found // 256, found % 256
    return (group % 2) * 1024 + (within // 16) * 64 + (group // 2) * 16 + within % 16


def local(
    vit_input,
    image_lengths,
    positions,
    vit_ln_gain,
    w_qkv,
    w_proj,
    merger_ln_gain,
    merger_w1,
    merger_w2,
    norm_gain,
    gate_up_weight,
    down_weight,
):
    tp_size = lax.axis_size(TP)
    seq_size = lax.axis_size("seq")
    own_patches = vit_input.shape[0]
    patch_width = vit_input.shape[1]
    head_cols = w_qkv.shape[2]
    local_heads = head_cols // HD
    normed_patches = layer_norm(vit_input.astype(jnp.float32), vit_ln_gain).astype(jnp.bfloat16)
    w_qkv_flat = w_qkv.reshape(patch_width, 3 * head_cols)
    projected = jnp.dot(
        plane_gather(normed_patches, 1, True).reshape(-1, patch_width), w_qkv_flat, preferred_element_type=jnp.float32
    ).astype(jnp.bfloat16)
    group_patches = projected.shape[0]
    projected = projected.reshape(group_patches, 3, local_heads, HD)
    image_index = image_ids(image_lengths[0], group_patches)
    attended = attend(projected[:, 0], projected[:, 1], projected[:, 2], image_index).reshape(
        group_patches, head_cols
    )
    picked = attended
    shares = jnp.dot(picked, w_proj, preferred_element_type=jnp.float32).astype(jnp.bfloat16)
    attn_sum = plane_reduce(shares.reshape(tp_size, own_patches, patch_width), 2, True, jnp.float32)
    vit_out = vit_input.astype(jnp.float32) + attn_sum
    own_tokens = own_patches // 4
    merged_in = (
        layer_norm(vit_out, merger_ln_gain)
        .astype(jnp.bfloat16)
        .reshape(own_tokens, 4 * patch_width)
    )
    expanded = jax.nn.gelu(
        jnp.dot(plane_gather(merged_in, 3, False).reshape(-1, 4 * patch_width), merger_w1, preferred_element_type=jnp.float32),
        approximate=False,
    ).astype(jnp.bfloat16)
    picked = expanded
    shares = jnp.dot(picked, merger_w2, preferred_element_type=jnp.float32).astype(jnp.bfloat16)
    everyone = all_tokens_of(shares.reshape(tp_size, own_tokens, D), 4).reshape(-1, WIDE)
    core = lax.rem(lax.axis_index("seq"), 2)
    own_tokens_of_core = jnp.take(everyone, sources(positions, core), axis=0).reshape(4, 256, WIDE)
    swap = [(i, i ^ 1) for i in range(seq_size)]
    gate_up_rows = jnp.transpose(gate_up_weight, (1, 2, 0))
    other_rows = lax.ppermute(gate_up_rows, "seq", swap)
    other_down = lax.ppermute(down_weight, "seq", swap)
    other_gain = lax.ppermute(norm_gain, "seq", swap)
    gain = jnp.where(
        core == 0, jnp.concatenate([norm_gain, other_gain]), jnp.concatenate([other_gain, norm_gain])
    )
    return feed_forward(
        own_tokens_of_core, gain[None], gate_up_rows, other_rows, down_weight, other_down, 5
    )


def solution(mesh):
    finer = Mesh(mesh.devices.reshape(mesh.shape["seq"], 4, 4), ("seq", "tp_0", "tp_1"))
    in_specs = (
        P(SEQ_TP, None),
        P("seq", None),
        P(),
        P(),
        P(None, None, TP),
        P(TP, None),
        P(),
        P(None, TP),
        P(TP, None),
        P("seq"),
        P("seq", None, TP),
        P(TP, "seq"),
    )
    out_specs = P(TP, "seq")
    return jax.shard_map(local, mesh=finer, in_specs=in_specs, out_specs=out_specs, check_vma=False)
```

```python
import functools
import jax
import jax.numpy as jnp
from jax import lax
from jax.experimental import pallas as pl
from jax.experimental.pallas import tpu as pltpu
from jax.sharding import Mesh
from jax.sharding import PartitionSpec as P

D = 8192
HD = 80
TP = ("tp_0", "tp_1")
SEQ_TP = ("seq", "tp_0", "tp_1")

MESH_ID = pl.DeviceIdType.MESH
AXES = ("tp_0", "tp_1")


def ring(axis, step):
    return {axis: lax.rem(lax.axis_index(axis) + step, 4)}


def remote(src, dst, send, recv, target):
    return pltpu.make_async_remote_copy(
        src_ref=src, dst_ref=dst, send_sem=send, recv_sem=recv, device_id=target, device_id_type=MESH_ID
    )


def greet(targets):
    barrier = pltpu.get_barrier_semaphore()
    for target in targets:
        pl.semaphore_signal(barrier, inc=1, device_id=target, device_id_type=MESH_ID)
    pl.semaphore_wait(barrier, len(targets))


def plane_neighbours():
    return [ring(axis, step) for axis in AXES for step in (1, 3)]


def gather_plane(own, slot, half_cut, quarter_cut, send, recv, forward=None):
    here = [lax.axis_index(axis) for axis in AXES]
    sent = []

    def index(half, first, second):
        offsets = (first, second) if half == 0 else (second, first)
        spots = [lax.rem(at + off, 4) for at, off in zip(here, offsets)]
        return spots[0] * 4 + spots[1]

    def place(half, first, second):
        return slot(index(half, first, second))

    def source(half, first, second):
        return own if (first, second) == (0, 0) else place(half, first, second)

    def start(half, phase, kind, axis, step, first, second, cut):
        at = half * 20 + phase * 4 + kind
        copy = remote(
            cut(source(half, first, second)), cut(place(half, first, second)), send.at[at], recv.at[at], ring(axis, step)
        )
        copy.start()
        sent.append(copy)

    def landed(half, phase, kind, axis, first, second, cut):
        at = half * 20 + phase * 4 + kind
        target = cut(place(half, first, second))
        remote(target, target, send.at[at], recv.at[at], ring(axis, 1)).wait_recv()
        if forward is not None:
            forward(at, lambda base: cut(base(index(half, first, second))))

    def axes(half):
        return (AXES[0], AXES[1]) if half == 0 else (AXES[1], AXES[0])

    def cuts(half):
        return (
            lambda ref: half_cut(ref, half),
            lambda ref: quarter_cut(ref, 2 * half),
            lambda ref: quarter_cut(ref, 2 * half + 1),
        )

    def spread(half, phase, first):
        whole, _, _ = cuts(half)
        axis = axes(half)[1]
        start(half, phase, 0, axis, 1, first, 0, whole)
        start(half, phase, 1, axis, 3, first, 0, whole)

    def relay(half, phase, first):
        whole, low, high = cuts(half)
        axis = axes(half)[1]
        landed(half, phase, 0, axis, first, 3, whole)
        start(half, phase, 2, axis, 1, first, 3, low)
        landed(half, phase, 1, axis, first, 1, whole)
        start(half, phase, 3, axis, 3, first, 1, high)

    def finish(half, phase, first):
        whole, low, high = cuts(half)
        axis = axes(half)[1]
        landed(half, phase, 2, axis, first, 2, low)
        landed(half, phase, 3, axis, first, 2, high)

    for half in (0, 1):
        whole, _, _ = cuts(half)
        start(half, 0, 0, axes(half)[0], 1, 0, 0, whole)
        start(half, 0, 1, axes(half)[0], 3, 0, 0, whole)
    for half in (0, 1):
        spread(half, 1, 0)
    for half in (0, 1):
        whole, low, high = cuts(half)
        axis = axes(half)[0]
        landed(half, 0, 0, axis, 3, 0, whole)
        start(half, 0, 2, axis, 1, 3, 0, low)
        spread(half, 2, 3)
        landed(half, 0, 1, axis, 1, 0, whole)
        start(half, 0, 3, axis, 3, 1, 0, high)
        spread(half, 3, 1)
    for half in (0, 1):
        relay(half, 1, 0)
    for half in (0, 1):
        whole, low, high = cuts(half)
        axis = axes(half)[0]
        landed(half, 0, 2, axis, 2, 0, low)
        landed(half, 0, 3, axis, 2, 0, high)
        spread(half, 4, 2)
    for phase, first in ((2, 3), (3, 1), (4, 2)):
        for half in (0, 1):
            relay(half, phase, first)
    for phase, first in ((1, 0), (2, 3), (3, 1), (4, 2)):
        for half in (0, 1):
            finish(half, phase, first)
    for copy in sent:
        copy.wait_send()


def reduce_plane(term, got, made, sums, send, recv, emit, eager=True):
    here = [lax.axis_index(axis) for axis in AXES]
    sent = []

    def axes(half):
        return (AXES[1], AXES[0]) if half == 0 else (AXES[0], AXES[1])

    def part(half, first, second, which):
        offsets = (first, second) if half == 0 else (second, first)
        spots = [lax.rem(at + off, 4) for at, off in zip(here, offsets)]
        return term(spots[0] * 4 + spots[1], 2 * half + which)

    def phase_source(half, phase):
        if phase < 4:
            return lambda offset, which: part(half, phase, offset, which)
        return lambda offset, which: sums.at[half * 8 + offset * 2 + which]

    def slot(half, phase, kind):
        return half * 30 + phase * 6 + kind

    def start(half, phase, kind, src, step):
        axis = axes(half)[0 if phase < 4 else 1]
        at = slot(half, phase, kind)
        copy = remote(src, got.at[at], send.at[at], recv.at[at], ring(axis, step))
        copy.start()
        sent.append(copy)

    def landed(half, phase, kind):
        at = slot(half, phase, kind)
        axis = axes(half)[0 if phase < 4 else 1]
        remote(got.at[at], got.at[at], send.at[at], recv.at[at], ring(axis, 1)).wait_recv()
        return got[at].astype(jnp.float32)

    def raw(half, phase):
        own = phase_source(half, phase)
        start(half, phase, 0, own(2, 0), 1)
        start(half, phase, 3, own(2, 1), 3)
        start(half, phase, 1, own(1, 1), 1)
        start(half, phase, 4, own(3, 0), 3)

    def summed(half, phase):
        own = phase_source(half, phase)
        for kind, offset, which, step in ((0, 1, 0, 1), (3, 3, 1, 3)):
            at = half * 10 + phase * 2 + which
            made[at] = (own(offset, which)[...].astype(jnp.float32) + landed(half, phase, kind)).astype(made.dtype)
            start(half, phase, kind + 2, made.at[at], step)

    def total(half, phase):
        own = phase_source(half, phase)
        return [
            own(0, which)[...].astype(jnp.float32) + landed(half, phase, near) + landed(half, phase, far)
            for which, near, far in ((0, 4, 2), (1, 1, 5))
        ]

    def settle(half, phase):
        for which, value in enumerate(total(half, phase)):
            sums[half * 8 + phase * 2 + which] = value.astype(sums.dtype)

    order = (2, 1, 3, 0)
    both = (0, 1)

    def late(first):
        own = phase_source_of_last
        for half in both:
            source = own(half)
            if first == 2:
                start(half, 4, 0, source(2, 0), 1)
                start(half, 4, 3, source(2, 1), 3)
            if first == 1:
                start(half, 4, 1, source(1, 1), 1)
            if first == 3:
                start(half, 4, 4, source(3, 0), 3)

    def phase_source_of_last(half):
        return phase_source(half, 4)

    for half in both:
        raw(half, order[0])
    for half in both:
        raw(half, order[1])
    if not eager:
        for phase in order[2:]:
            for half in both:
                raw(half, phase)
    yield
    for at, phase in enumerate(order):
        for half in both:
            summed(half, phase)
        if eager and at + 2 < 4:
            for half in both:
                raw(half, order[at + 2])
        if eager and at >= 1:
            for half in both:
                settle(half, order[at - 1])
            late(order[at - 1])
    yield
    if not eager:
        for phase in order[:3]:
            for half in both:
                settle(half, phase)
            late(phase)
    yield
    for half in both:
        summed(half, 4)
    yield
    for half in both:
        settle(half, 0)
    for half in both:
        for which, value in enumerate(total(half, 4)):
            emit(2 * half + which, value)
    for copy in sent:
        copy.wait_send()


def run(steps):
    for _ in steps:
        pass


def cut_rows(ref, begin, size):
    return ref.at[pl.ds(begin, size)]


def plane_gather(block, collective_id, by_rows):
    rows, cols = block.shape

    def cutter(share):
        def cut(ref, at):
            if by_rows:
                return ref.at[pl.ds(at * (rows // share), rows // share), :]
            return ref.at[:, pl.ds(at * (cols // share), cols // share)]
        return cut

    def kernel(own, out, send, recv):
        greet(plane_neighbours())
        me = lax.axis_index("tp_0") * 4 + lax.axis_index("tp_1")
        out[me] = own[...]
        gather_plane(own, lambda t: out.at[t], cutter(2), cutter(4), send, recv)

    return pl.pallas_call(
        kernel,
        out_shape=jax.ShapeDtypeStruct((16, rows, cols), block.dtype),
        in_specs=[pl.BlockSpec(memory_space=pltpu.VMEM)],
        out_specs=pl.BlockSpec(memory_space=pltpu.VMEM),
        scratch_shapes=[pltpu.SemaphoreType.DMA((40,)), pltpu.SemaphoreType.DMA((40,))],
        compiler_params=pltpu.CompilerParams(collective_id=collective_id, has_side_effects=True),
        name=f"plane_gather_{collective_id}",
    )(block)


def plane_reduce(terms, collective_id, by_rows, out_dtype):
    _, rows, cols = terms.shape
    quarter = (rows // 4, cols) if by_rows else (rows, cols // 4)

    def cut(ref, at):
        if by_rows:
            return ref.at[pl.ds(at * quarter[0], quarter[0]), :]
        return ref.at[:, pl.ds(at * quarter[1], quarter[1])]

    def kernel(terms_ref, out, got, made, sums, send, recv):
        greet(plane_neighbours())

        def emit(at, value):
            cut(out, at)[...] = value.astype(out.dtype)

        run(reduce_plane(lambda t, at: cut(terms_ref.at[t], at), got, made, sums, send, recv, emit))

    return pl.pallas_call(
        kernel,
        out_shape=jax.ShapeDtypeStruct((rows, cols), out_dtype),
        in_specs=[pl.BlockSpec(memory_space=pltpu.VMEM)],
        out_specs=pl.BlockSpec(memory_space=pltpu.VMEM),
        scratch_shapes=[
            pltpu.VMEM((60, *quarter), terms.dtype),
            pltpu.VMEM((20, *quarter), terms.dtype),
            pltpu.VMEM((16, *quarter), terms.dtype),
            pltpu.SemaphoreType.DMA((60,)),
            pltpu.SemaphoreType.DMA((60,)),
        ],
        compiler_params=pltpu.CompilerParams(collective_id=collective_id, has_side_effects=True),
        name=f"plane_reduce_{collective_id}",
    )(terms)
WIDE = 2176
PADDED = 1920


def along_x(step):
    seq = lax.axis_index("seq")
    return {"seq": lax.rem(seq + 2 * step, 8)}


def partner():
    seq = lax.axis_index("seq")
    return {"seq": seq + 1 - 2 * lax.rem(seq, 2)}


def token_kernel(terms_ref, out, got, made, sums, vis, parcels, block, send, recv, xsend, xrecv, gsend, grecv, dsend, drecv):
    greet(plane_neighbours() + [along_x(step) for step in (1, 2, 3)] + [partner()])
    seq = lax.axis_index("seq")
    x, core = seq // 2, lax.rem(seq, 2)
    me = lax.axis_index("tp_0") * 4 + lax.axis_index("tp_1")

    def emit(at, value):
        parcels[at, :, :2048] = value.astype(jnp.bfloat16)

    run(reduce_plane(lambda t, at: terms_ref.at[t, :, pl.ds(at * 2048, 2048)], got, made, sums, send, recv, emit))
    squares = jnp.zeros((16, 1), jnp.float32)
    for at in range(4):
        values = parcels[at, :, :2048].astype(jnp.float32)
        squares = squares + jnp.sum(values * values, axis=1, keepdims=True)
    high = squares.astype(jnp.bfloat16).astype(jnp.float32)
    low = squares - high
    lane = lax.broadcasted_iota(jnp.int32, (16, 128), 1)
    tail = jnp.where(lane == 0, high, jnp.where(lane == 1, low, 0.0)).astype(jnp.bfloat16)
    for at in range(4):
        parcels[at, :, 2048:] = tail
    mine = pl.ds(pl.multiple_of(x * 16, 16), 16)
    sent = []
    for step in (2, 1, 3):
        copy = remote(
            parcels.at[lax.rem(x + step, 4)], block.at[mine, :], xsend.at[step], xrecv.at[step], along_x(step)
        )
        copy.start()
        sent.append(copy)
    block[mine, :] = parcels[x]
    for step in (1, 3, 2):
        rows = pl.ds(pl.multiple_of(lax.rem(x + 4 - step, 4) * 16, 16), 16)
        landing = block.at[rows, :]
        remote(landing, landing, xsend.at[step], xrecv.at[step], along_x(step)).wait_recv()
    for copy in sent:
        copy.wait_send()
    forwarded = []
    expected = []

    def forward(at, view):
        piece = view(lambda t: out.at[core, t])
        copy = remote(piece, piece, dsend.at[at], drecv.at[at], partner())
        copy.start()
        forwarded.append(copy)
        other = view(lambda t: out.at[1 - core, t])
        expected.append(remote(other, other, dsend.at[at], drecv.at[at], partner()))

    own_copy = remote(block, out.at[core, me], dsend.at[40], drecv.at[40], partner())
    own_copy.start()
    out[core, me] = block[...]
    gather_plane(
        block,
        lambda t: out.at[core, t],
        lambda ref, half: ref.at[pl.ds(half * 32, 32), :],
        lambda ref, at: ref.at[pl.ds(at * 16, 16), :],
        gsend,
        grecv,
        forward,
    )
    other = out.at[1 - core, me]
    expected.append(remote(other, other, dsend.at[40], drecv.at[40], partner()))
    own_copy.wait_send()
    for copy in forwarded:
        copy.wait_send()
    for copy in expected:
        copy.wait_recv()


def all_tokens_of(terms, collective_id):
    return pl.pallas_call(
        token_kernel,
        out_shape=jax.ShapeDtypeStruct((2, 16, 64, WIDE), jnp.bfloat16),
        in_specs=[pl.BlockSpec(memory_space=pltpu.VMEM)],
        out_specs=pl.BlockSpec(memory_space=pltpu.VMEM),
        scratch_shapes=[
            pltpu.VMEM((60, 16, 2048), jnp.bfloat16),
            pltpu.VMEM((20, 16, 2048), jnp.bfloat16),
            pltpu.VMEM((16, 16, 2048), jnp.bfloat16),
            pltpu.VMEM((8, 128), jnp.float32),
            pltpu.VMEM((4, 16, WIDE), jnp.bfloat16),
            pltpu.VMEM((64, WIDE), jnp.bfloat16),
            pltpu.SemaphoreType.DMA((60,)),
            pltpu.SemaphoreType.DMA((60,)),
            pltpu.SemaphoreType.DMA((4,)),
            pltpu.SemaphoreType.DMA((4,)),
            pltpu.SemaphoreType.DMA((40,)),
            pltpu.SemaphoreType.DMA((40,)),
            pltpu.SemaphoreType.DMA((41,)),
            pltpu.SemaphoreType.DMA((41,)),
        ],
        compiler_params=pltpu.CompilerParams(
            collective_id=collective_id, has_side_effects=True, vmem_limit_bytes=48 * 1024 * 1024
        ),
        name="all_tokens",
    )(terms)


GROUPS = ((0, 1024), (1024, 896))
BLOCKS = (((0, 0), (0, 1)), ((1, 1), (3, 0)), ((2, 0), (2, 1)), ((1, 0), (3, 1)))


def feed_forward_kernel(
    everyone, slots, gain, w_own, w_other, d_own, d_other, out,
    weights, downs, picks, raw, rows, strip, parts, came, hidden, got, made, sums, fin,
    wsem, osem, psend, precv, hsend, hrecv, send, recv, fsend, frecv,
):
    seq = lax.axis_index("seq")
    x, core = seq // 2, lax.rem(seq, 2)
    me = lax.axis_index("tp_0") * 4 + lax.axis_index("tp_1")
    real = w_own.shape[1]
    weights[:, pl.ds(1840, 80), :] = jnp.zeros((2, 80, 2048), jnp.bfloat16)
    downs[pl.ds(1840, 80), :] = jnp.zeros((80, 2048), jnp.bfloat16)
    sides = ((w_own, d_own, core), (w_other, d_other, 1 - core))

    def weight_copies(n):
        size = 256 if n < 7 else real - 1792
        return [
            pltpu.make_async_copy(
                w.at[:, pl.ds(n * 256, size), :],
                weights.at[:, pl.ds(n * 256, size), pl.ds(pl.multiple_of(at * 1024, 1024), 1024)],
                wsem.at[n, side],
            )
            for side, (w, _, at) in enumerate(sides)
        ]

    def down_copies():
        return [
            pltpu.make_async_copy(
                d, downs.at[pl.ds(0, real), pl.ds(pl.multiple_of(at * 1024, 1024), 1024)], osem.at[side]
            )
            for side, (_, d, at) in enumerate(sides)
        ]

    for n in range(8):
        for copy in weight_copies(n):
            copy.start()
    for copy in down_copies():
        copy.start()
    strip[...] = jnp.zeros_like(strip)

    def owner(step):
        return lax.rem(x + step, 4)

    def pick(block):
        upper, lower = BLOCKS[block]
        row = lax.broadcasted_iota(jnp.int32, (256, 1), 0)
        top = row < 128
        at = jnp.where(top, owner(upper[0]), owner(lower[0]))
        row = jnp.where(top, row + upper[1] * 128, row - 128 + lower[1] * 128)
        slot = (row // 16) * 128 + core * 64 + at * 16 + row % 16
        picks[...] = jnp.where(slots[...] == slot, 1.0, 0.0).astype(jnp.bfloat16)

        def piece(begin, size):
            value = jnp.dot(picks[...], everyone[:, pl.ds(begin, size)], preferred_element_type=jnp.float32)
            raw[:, pl.ds(begin, size)] = value.astype(jnp.bfloat16)

        @pl.loop(0, 8)
        def _(n):
            piece(pl.multiple_of(n * 256, 256), 256)

        piece(2048, 128)
        square = raw[:, 2048:2049].astype(jnp.float32) + raw[:, 2049:2050].astype(jnp.float32)
        inverse = lax.rsqrt(square / D + 1e-06)
        rows[...] = (raw[:, :2048].astype(jnp.float32) * inverse * gain[...]).astype(jnp.bfloat16)
        for base, (step, half) in zip((0, 128), (upper, lower)):
            found = raw[pl.ds(pl.multiple_of(base + lax.rem(me, 8) * 16, 16), 16), :2048]
            here = me // 8 == half
            strip[step] = jnp.where(here, found, strip[step])

    def multiply(step, group, first=False):
        def piece(begin, size):
            for half in range(2):
                value = lax.dot_general(
                    rows[...], weights[half, pl.ds(begin, size), :], (((1,), (1,)), ((), ())),
                    preferred_element_type=jnp.float32,
                )
                parts[step, half, :, pl.ds(begin, size)] = value.astype(jnp.bfloat16)

        if first:
            for n in range(4 * group, 4 * group + 4):
                for copy in weight_copies(n):
                    copy.wait()
        full = 4 if group == 0 else 3

        @pl.loop(0, full)
        def _(n):
            piece(pl.multiple_of(GROUPS[group][0] + n * 256, 256), 256)

        if group == 1:
            piece(1792, 128)

    def cut(ref, sub):
        begin, size = GROUPS[sub % 2]
        return ref.at[:, pl.ds(sub // 2 * 128, 128), pl.ds(begin, size)]

    sent = []

    def part_slot(kind, index):
        return came.at[kind * 2 + index, :, :, pl.ds(0, GROUPS[index][1])]

    part_sends = {}

    def pass_part(kind, index, src, way, step):
        at = kind * 2 + index
        copy = remote(src, part_slot(kind, index), psend.at[at], precv.at[at], along_x(way))
        copy.start()
        part_sends.setdefault(step, []).append(copy)

    def part_landed(kind, index):
        at = kind * 2 + index
        landing = part_slot(kind, index)
        remote(landing, landing, psend.at[at], precv.at[at], along_x(1)).wait_recv()
        return landing

    pick(2)
    for index in range(2):
        multiply(2, index, True)
        if index == 0:
            greet(plane_neighbours() + [along_x(step) for step in (1, 3)] + [partner()])
        pass_part(0, index, cut(parts.at[2], index), 1, 2)
        pass_part(3, index, cut(parts.at[2], 2 + index), 3, 2)
    pick(1)
    for index in range(2):
        multiply(1, index)
        pass_part(1, index, cut(parts.at[1], index), 1, 1)
        pass_part(4, index, cut(parts.at[1], 2 + index), 3, 1)
    pick(3)
    for index in range(2):
        multiply(3, index)
        for kind, sub, way in ((0, index, 1), (3, 2 + index, 3)):
            arrived = part_landed(kind, index)
            target = cut(parts.at[3], sub)
            target[...] = (target[...].astype(jnp.float32) + arrived[...].astype(jnp.float32)).astype(jnp.bfloat16)
            pass_part(kind + 2, index, target, way, 3)
    pick(0)
    for index in range(2):
        multiply(0, index)

    def hidden_piece(step, sub):
        begin, size = GROUPS[sub % 2]
        return hidden.at[owner(step), pl.ds(sub // 2 * 128, 128), pl.ds(begin, size)]

    def pass_hidden(at, piece, step):
        copy = remote(piece, piece, hsend.at[at], hrecv.at[at], along_x(step))
        copy.start()
        sent.append(copy)

    def hidden_landed(at, piece):
        remote(piece, piece, hsend.at[at], hrecv.at[at], along_x(1)).wait_recv()

    for index in range(2):
        for sub, near, far in ((index, 4, 2), (2 + index, 1, 5)):
            one = part_landed(near, index)
            two = part_landed(far, index)
            own = cut(parts.at[0], sub)
            gate, up = [
                own[half].astype(jnp.float32) + one[half].astype(jnp.float32) + two[half].astype(jnp.float32)
                for half in range(2)
            ]
            piece = hidden_piece(0, sub)
            piece[...] = (gate / (1.0 + jnp.exp(-gate)) * up).astype(jnp.bfloat16)
            pass_hidden(sub, piece, 1)
            pass_hidden(4 + sub, piece, 3)
    for copy in down_copies():
        copy.wait()

    def project(step):
        at = owner(step)
        for copy in part_sends.get(step, []):
            copy.wait_send()
        for side in range(2):
            @pl.loop(0, 4)
            def _(n):
                begin = pl.multiple_of(n * 256, 256)
                value = jnp.dot(
                    hidden[at],
                    downs[:, pl.ds(pl.multiple_of(side * 1024 + begin, 256), 256)],
                    preferred_element_type=jnp.float32,
                )
                parts[step, side, :, pl.ds(begin, 256)] = value.astype(jnp.bfloat16)

    def reduction(step):
        def term(t, at):
            return parts.at[step, at // 2, pl.ds(pl.multiple_of(t * 16, 16), 16), pl.ds(at % 2 * 512, 512)]

        def emit(at, value):
            total = value + strip[step, :, pl.ds(at * 512, 512)].astype(jnp.float32)
            target = pl.ds(pl.multiple_of(owner(step) * 16, 16), 16)
            fin[at // 2, target, pl.ds(at % 2 * 512, 512)] = total.astype(jnp.bfloat16)

        return reduce_plane(
            term, got.at[step], made.at[step], sums.at[step], send.at[step], recv.at[step], emit, False
        )

    def relay(index):
        hidden_landed(index, hidden_piece(3, index))
        pass_hidden(8 + index, hidden_piece(3, index), 1)
        hidden_landed(4 + 2 + index, hidden_piece(1, 2 + index))
        pass_hidden(10 + index, hidden_piece(1, 2 + index), 3)

    flows = {step: reduction(step) for step in range(4)}
    project(0)
    next(flows[0])
    relay(0)
    next(flows[0])
    relay(1)
    next(flows[0])
    for index in range(2):
        hidden_landed(2 + index, hidden_piece(3, 2 + index))
    project(3)
    next(flows[3])
    for index in range(2):
        hidden_landed(4 + index, hidden_piece(1, index))
    project(1)
    next(flows[1])
    next(flows[0])
    next(flows[3])
    next(flows[1])
    for index in range(2):
        hidden_landed(8 + index, hidden_piece(2, index))
        hidden_landed(10 + index, hidden_piece(2, 2 + index))
    project(2)
    next(flows[2])
    next(flows[3])
    next(flows[1])
    next(flows[2])
    next(flows[3])
    next(flows[1])
    next(flows[2])
    run(flows[0])
    run(flows[3])
    run(flows[1])
    run(flows[2])
    mine = pl.ds(pl.multiple_of(core * 64, 64), 64)
    theirs = pl.ds(pl.multiple_of((1 - core) * 64, 64), 64)
    swap = remote(fin.at[1 - core], out.at[mine, :], fsend, frecv, partner())
    swap.start()
    out[mine, :] = fin[core]
    swap.wait_send()
    landing = out.at[theirs, :]
    remote(landing, landing, fsend, frecv, partner()).wait_recv()
    for copy in sent + part_sends.get(0, []):
        copy.wait_send()


def feed_forward(everyone, slots, gain, w_own, w_other, d_own, d_other, collective_id):
    anywhere = pl.BlockSpec(memory_space=pl.ANY)
    vmem = pl.BlockSpec(memory_space=pltpu.VMEM)
    dma = pltpu.SemaphoreType.DMA
    bf16 = jnp.bfloat16
    return pl.pallas_call(
        feed_forward_kernel,
        out_shape=jax.ShapeDtypeStruct((128, 1024), bf16),
        in_specs=[vmem, vmem, vmem, anywhere, anywhere, anywhere, anywhere],
        out_specs=vmem,
        scratch_shapes=[
            pltpu.VMEM((2, PADDED, 2048), bf16),
            pltpu.VMEM((PADDED, 2048), bf16),
            pltpu.VMEM((256, 2048), bf16),
            pltpu.VMEM((256, WIDE), bf16),
            pltpu.VMEM((256, 2048), bf16),
            pltpu.VMEM((4, 16, 2048), bf16),
            pltpu.VMEM((4, 2, 256, PADDED), bf16),
            pltpu.VMEM((12, 2, 128, 1024), bf16),
            pltpu.VMEM((4, 256, PADDED), bf16),
            pltpu.VMEM((4, 60, 16, 512), bf16),
            pltpu.VMEM((4, 20, 16, 512), bf16),
            pltpu.VMEM((4, 16, 16, 512), bf16),
            pltpu.VMEM((2, 64, 1024), bf16),
            dma((8, 2)),
            dma((2,)),
            dma((12,)),
            dma((12,)),
            dma((12,)),
            dma((12,)),
            dma((4, 60)),
            dma((4, 60)),
            dma,
            dma,
        ],
        compiler_params=pltpu.CompilerParams(
            collective_id=collective_id, has_side_effects=True, vmem_limit_bytes=67043328
        ),
        name="feed_forward",
    )(everyone, slots, gain, w_own, w_other, d_own, d_other)


def layer_norm(values, gain):
    mean = jnp.mean(values, axis=-1, keepdims=True)
    centered = values - mean
    variance = jnp.mean(centered * centered, axis=-1, keepdims=True)
    return centered * lax.rsqrt(variance + 1e-06) * gain


def image_ids(lengths, count):
    image_ends = jnp.cumsum(lengths) * 4
    patch_index = jnp.arange(count, dtype=jnp.int32)
    return jnp.sum((patch_index[:, None] >= image_ends[None, :]).astype(jnp.int32), axis=1)


def attend(query, keys, values, image_index):
    scores = jnp.einsum("qhe,khe->hqk", query, keys, preferred_element_type=jnp.float32) * HD ** (
        -0.5
    )
    same_image = image_index[:, None] == image_index[None, :]
    scores = jnp.where(same_image[None], scores, -1e30)
    top = jnp.max(scores, axis=-1, keepdims=True)
    expo = jnp.exp(scores - top)
    weights = (expo / jnp.sum(expo, axis=-1, keepdims=True)).astype(jnp.bfloat16)
    output = jnp.einsum("hqk,khe->qhe", weights, values, preferred_element_type=jnp.float32)
    return output.astype(jnp.bfloat16)


def local(
    vit_input,
    image_lengths,
    positions,
    vit_ln_gain,
    w_qkv,
    w_proj,
    merger_ln_gain,
    merger_w1,
    merger_w2,
    norm_gain,
    gate_up_weight,
    down_weight,
):
    tp_size = lax.axis_size(TP)
    seq_size = lax.axis_size("seq")
    own_patches = vit_input.shape[0]
    patch_width = vit_input.shape[1]
    head_cols = w_qkv.shape[2]
    local_heads = head_cols // HD
    normed_patches = layer_norm(vit_input.astype(jnp.float32), vit_ln_gain).astype(jnp.bfloat16)
    w_qkv_flat = w_qkv.reshape(patch_width, 3 * head_cols)
    projected = jnp.dot(
        plane_gather(normed_patches, 1, True).reshape(-1, patch_width), w_qkv_flat, preferred_element_type=jnp.float32
    ).astype(jnp.bfloat16)
    group_patches = projected.shape[0]
    projected = projected.reshape(group_patches, 3, local_heads, HD)
    image_index = image_ids(image_lengths[0], group_patches)
    attended = attend(projected[:, 0], projected[:, 1], projected[:, 2], image_index).reshape(
        group_patches, head_cols
    )
    picked = attended
    shares = jnp.dot(picked, w_proj, preferred_element_type=jnp.float32).astype(jnp.bfloat16)
    attn_sum = plane_reduce(shares.reshape(tp_size, own_patches, patch_width), 2, True, jnp.float32)
    vit_out = vit_input.astype(jnp.float32) + attn_sum
    own_tokens = own_patches // 4
    merged_in = (
        layer_norm(vit_out, merger_ln_gain)
        .astype(jnp.bfloat16)
        .reshape(own_tokens, 4 * patch_width)
    )
    expanded = jax.nn.gelu(
        jnp.dot(plane_gather(merged_in, 3, False).reshape(-1, 4 * patch_width), merger_w1, preferred_element_type=jnp.float32),
        approximate=False,
    ).astype(jnp.bfloat16)
    picked = expanded
    shares = jnp.dot(picked, merger_w2, preferred_element_type=jnp.float32).astype(jnp.bfloat16)
    everyone = all_tokens_of(shares.reshape(tp_size, own_tokens, D), 4).reshape(-1, WIDE)
    core = lax.rem(lax.axis_index("seq"), 2)
    slots = positions.reshape(4, 2, 16, 16).transpose(1, 2, 0, 3).reshape(1, -1)
    swap = [(i, i ^ 1) for i in range(seq_size)]
    gate_up_rows = jnp.transpose(gate_up_weight, (1, 2, 0))
    other_rows = lax.ppermute(gate_up_rows, "seq", swap)
    other_down = lax.ppermute(down_weight, "seq", swap)
    other_gain = lax.ppermute(norm_gain, "seq", swap)
    gain = jnp.where(
        core == 0, jnp.concatenate([norm_gain, other_gain]), jnp.concatenate([other_gain, norm_gain])
    )
    return feed_forward(
        everyone, slots, gain[None], gate_up_rows, other_rows, down_weight, other_down, 5
    )


def solution(mesh):
    finer = Mesh(mesh.devices.reshape(mesh.shape["seq"], 4, 4), ("seq", "tp_0", "tp_1"))
    in_specs = (
        P(SEQ_TP, None),
        P("seq", None),
        P(),
        P(),
        P(None, None, TP),
        P(TP, None),
        P(),
        P(None, TP),
        P(TP, None),
        P("seq"),
        P("seq", None, TP),
        P(TP, "seq"),
    )
    out_specs = P(TP, "seq")
    return jax.shard_map(local, mesh=finer, in_specs=in_specs, out_specs=out_specs, check_vma=False)
```

```python
import jax
import jax.numpy as jnp
from jax import lax
from jax.experimental import pallas as pl
from jax.experimental.pallas import tpu as pltpu
from jax.sharding import Mesh
from jax.sharding import PartitionSpec as P

D = 8192
HD = 80
TP = ("tp_0", "tp_1")
SEQ_TP = ("seq", "tp_0", "tp_1")

MESH_ID = pl.DeviceIdType.MESH
AXES = ("tp_0", "tp_1")


def ring(axis, step):
    return {axis: lax.rem(lax.axis_index(axis) + step, 4)}


def remote(src, dst, send, recv, target):
    return pltpu.make_async_remote_copy(
        src_ref=src, dst_ref=dst, send_sem=send, recv_sem=recv, device_id=target, device_id_type=MESH_ID
    )


def greet(targets):
    barrier = pltpu.get_barrier_semaphore()
    for target in targets:
        pl.semaphore_signal(barrier, inc=1, device_id=target, device_id_type=MESH_ID)
    pl.semaphore_wait(barrier, len(targets))


def plane_neighbours():
    return [ring(axis, step) for axis in AXES for step in (1, 3)]


def gather_plane(own, slot, half_cut, quarter_cut, send, recv, forward=None):
    here = [lax.axis_index(axis) for axis in AXES]
    sent = []

    def index(half, first, second):
        offsets = (first, second) if half == 0 else (second, first)
        spots = [lax.rem(at + off, 4) for at, off in zip(here, offsets)]
        return spots[0] * 4 + spots[1]

    def place(half, first, second):
        return slot(index(half, first, second))

    def source(half, first, second):
        return own if (first, second) == (0, 0) else place(half, first, second)

    def start(half, phase, kind, axis, step, first, second, cut):
        at = half * 20 + phase * 4 + kind
        copy = remote(
            cut(source(half, first, second)), cut(place(half, first, second)), send.at[at], recv.at[at], ring(axis, step)
        )
        copy.start()
        sent.append(copy)

    def landed(half, phase, kind, axis, first, second, cut):
        at = half * 20 + phase * 4 + kind
        target = cut(place(half, first, second))
        remote(target, target, send.at[at], recv.at[at], ring(axis, 1)).wait_recv()
        if forward is not None:
            forward(at, lambda base: cut(base(index(half, first, second))))

    def axes(half):
        return (AXES[0], AXES[1]) if half == 0 else (AXES[1], AXES[0])

    def cuts(half):
        return (
            lambda ref: half_cut(ref, half),
            lambda ref: quarter_cut(ref, 2 * half),
            lambda ref: quarter_cut(ref, 2 * half + 1),
        )

    def spread(half, phase, first):
        whole, _, _ = cuts(half)
        axis = axes(half)[1]
        start(half, phase, 0, axis, 1, first, 0, whole)
        start(half, phase, 1, axis, 3, first, 0, whole)

    def relay(half, phase, first):
        whole, low, high = cuts(half)
        axis = axes(half)[1]
        landed(half, phase, 0, axis, first, 3, whole)
        start(half, phase, 2, axis, 1, first, 3, low)
        landed(half, phase, 1, axis, first, 1, whole)
        start(half, phase, 3, axis, 3, first, 1, high)

    def finish(half, phase, first):
        whole, low, high = cuts(half)
        axis = axes(half)[1]
        landed(half, phase, 2, axis, first, 2, low)
        landed(half, phase, 3, axis, first, 2, high)

    for half in (0, 1):
        whole, _, _ = cuts(half)
        start(half, 0, 0, axes(half)[0], 1, 0, 0, whole)
        start(half, 0, 1, axes(half)[0], 3, 0, 0, whole)
    for half in (0, 1):
        spread(half, 1, 0)
    yield
    for half in (0, 1):
        whole, low, high = cuts(half)
        axis = axes(half)[0]
        landed(half, 0, 0, axis, 3, 0, whole)
        start(half, 0, 2, axis, 1, 3, 0, low)
        spread(half, 2, 3)
        landed(half, 0, 1, axis, 1, 0, whole)
        start(half, 0, 3, axis, 3, 1, 0, high)
        spread(half, 3, 1)
    yield
    for half in (0, 1):
        relay(half, 1, 0)
    yield
    for half in (0, 1):
        whole, low, high = cuts(half)
        axis = axes(half)[0]
        landed(half, 0, 2, axis, 2, 0, low)
        landed(half, 0, 3, axis, 2, 0, high)
        spread(half, 4, 2)
    yield
    for phase, first in ((2, 3), (3, 1), (4, 2)):
        for half in (0, 1):
            relay(half, phase, first)
    yield
    for phase, first in ((1, 0), (2, 3), (3, 1), (4, 2)):
        for half in (0, 1):
            finish(half, phase, first)
    for copy in sent:
        copy.wait_send()


def reduce_plane(term, got, made, sums, send, recv, emit, eager=True):
    here = [lax.axis_index(axis) for axis in AXES]
    sent = []

    def axes(half):
        return (AXES[1], AXES[0]) if half == 0 else (AXES[0], AXES[1])

    def part(half, first, second, which):
        offsets = (first, second) if half == 0 else (second, first)
        spots = [lax.rem(at + off, 4) for at, off in zip(here, offsets)]
        return term(spots[0] * 4 + spots[1], 2 * half + which)

    def phase_source(half, phase):
        if phase < 4:
            return lambda offset, which: part(half, phase, offset, which)
        return lambda offset, which: sums.at[half * 8 + offset * 2 + which]

    def slot(half, phase, kind):
        return half * 30 + phase * 6 + kind

    def start(half, phase, kind, src, step):
        axis = axes(half)[0 if phase < 4 else 1]
        at = slot(half, phase, kind)
        copy = remote(src, got.at[at], send.at[at], recv.at[at], ring(axis, step))
        copy.start()
        sent.append(copy)

    def landed(half, phase, kind):
        at = slot(half, phase, kind)
        axis = axes(half)[0 if phase < 4 else 1]
        remote(got.at[at], got.at[at], send.at[at], recv.at[at], ring(axis, 1)).wait_recv()
        return got[at].astype(jnp.float32)

    def raw(half, phase):
        own = phase_source(half, phase)
        start(half, phase, 0, own(2, 0), 1)
        start(half, phase, 3, own(2, 1), 3)
        start(half, phase, 1, own(1, 1), 1)
        start(half, phase, 4, own(3, 0), 3)

    def summed(half, phase):
        own = phase_source(half, phase)
        for kind, offset, which, step in ((0, 1, 0, 1), (3, 3, 1, 3)):
            at = half * 10 + phase * 2 + which
            made[at] = (own(offset, which)[...].astype(jnp.float32) + landed(half, phase, kind)).astype(made.dtype)
            start(half, phase, kind + 2, made.at[at], step)

    def total(half, phase):
        own = phase_source(half, phase)
        return [
            own(0, which)[...].astype(jnp.float32) + landed(half, phase, near) + landed(half, phase, far)
            for which, near, far in ((0, 4, 2), (1, 1, 5))
        ]

    def settle(half, phase):
        for which, value in enumerate(total(half, phase)):
            sums[half * 8 + phase * 2 + which] = value.astype(sums.dtype)

    order = (2, 1, 3, 0)
    both = (0, 1)

    def late(first):
        own = phase_source_of_last
        for half in both:
            source = own(half)
            if first == 2:
                start(half, 4, 0, source(2, 0), 1)
                start(half, 4, 3, source(2, 1), 3)
            if first == 1:
                start(half, 4, 1, source(1, 1), 1)
            if first == 3:
                start(half, 4, 4, source(3, 0), 3)

    def phase_source_of_last(half):
        return phase_source(half, 4)

    for half in both:
        raw(half, order[0])
    for half in both:
        raw(half, order[1])
    if not eager:
        for phase in order[2:]:
            for half in both:
                raw(half, phase)
    yield
    for at, phase in enumerate(order):
        for half in both:
            summed(half, phase)
        if eager and at + 2 < 4:
            for half in both:
                raw(half, order[at + 2])
        if eager and at >= 1:
            for half in both:
                settle(half, order[at - 1])
            late(order[at - 1])
    yield
    if not eager:
        for phase in order[:3]:
            for half in both:
                settle(half, phase)
            late(phase)
    yield
    for half in both:
        summed(half, 4)
    yield
    for half in both:
        settle(half, 0)
    for half in both:
        for which, value in enumerate(total(half, 4)):
            emit(2 * half + which, value)
    for copy in sent:
        copy.wait_send()


def run(steps):
    for _ in steps:
        pass
WIDE = 2176
PADDED = 1920


def along_x(step):
    seq = lax.axis_index("seq")
    return {"seq": lax.rem(seq + 2 * step, 8)}


def partner():
    seq = lax.axis_index("seq")
    return {"seq": seq + 1 - 2 * lax.rem(seq, 2)}


ROW_CUTS = ((0, 32), (32, 16), (48, 16), (64, 16))
ROW_HALVES = ((0, 48), (48, 32))


def share_with_partner(buffer, core, send, recv, sent, expected):
    def forward(at, view):
        piece = view(lambda t: buffer(core, t))
        copy = remote(piece, piece, send.at[at], recv.at[at], partner())
        copy.start()
        sent.append(copy)
        other = view(lambda t: buffer(1 - core, t))
        expected.append(remote(other, other, send.at[at], recv.at[at], partner()))

    return forward


def norm_rows(values, gain):
    mean = jnp.mean(values, axis=-1, keepdims=True)
    centered = values - mean
    variance = jnp.mean(centered * centered, axis=-1, keepdims=True)
    return centered * lax.rsqrt(variance + 1e-06) * gain


def vision_kernel(
    vit, ends, ln_gain, merger_gain, w_qkv, w_proj, w_one, w_two, out,
    own, patches, qkv, wq, wp, att, heads, lined, tiles, block_in, merged, one, expanded, two, terms,
    got, made, sums, parcels, block,
    wsem, asend, arecv, psend, precv, qsend, qrecv, hsend, hrecv, msend, mrecv,
    send, recv, xsend, xrecv, gsend, grecv, dsend, drecv,
):
    seq = lax.axis_index("seq")
    x, core = seq // 2, lax.rem(seq, 2)
    y, z = [lax.axis_index(axis) for axis in AXES]
    me = y * 4 + z
    others = [(dy, dz) for dy in range(4) for dz in range(4) if (dy, dz) != (0, 0)]

    def peer(dy, dz):
        return {"tp_0": lax.rem(y + dy, 4), "tp_1": lax.rem(z + dz, 4)}

    def peer_index(dy, dz):
        return lax.rem(y + dy, 4) * 4 + lax.rem(z + dz, 4)

    def proj_slot(side, t):
        return wp.at[t, :, pl.ds(pl.multiple_of(side * 640, 128), 640)]

    wq[:, pl.ds(80, 48), :] = jnp.zeros((3, 48, 1280), jnp.bfloat16)
    loads = [
        pltpu.make_async_copy(w_qkv, wq.at[:, pl.ds(0, 80), :], wsem.at[0]),
        pltpu.make_async_copy(w_proj, wp.at[me], wsem.at[1]),
        pltpu.make_async_copy(w_one, one, wsem.at[2]),
        pltpu.make_async_copy(w_two, two, wsem.at[3]),
    ]
    for copy in loads:
        copy.start()
    targets = [peer(*offset) for offset in others] + [along_x(step) for step in (1, 2, 3)] + [partner()]
    barrier = pltpu.get_barrier_semaphore()
    for target in targets:
        pl.semaphore_signal(barrier, inc=1, device_id=target, device_id_type=MESH_ID)
    own[...] = norm_rows(vit[...].astype(jnp.float32), ln_gain[...]).astype(jnp.bfloat16)
    pl.semaphore_wait(barrier, len(targets))

    rows_half = lambda ref, half: ref.at[pl.ds(half * 32, 32), :]
    rows_quarter = lambda ref, at: ref.at[pl.ds(at * 16, 16), :]
    patches[me] = own[...]
    run(gather_plane(own, lambda t: patches.at[t], rows_half, rows_quarter, asend, arecv))

    loads[1].wait()
    shared, awaited = [], []
    weights = gather_plane(
        proj_slot(core, me),
        lambda t: proj_slot(core, t),
        lambda ref, half: ref.at[pl.ds(*ROW_HALVES[half]), :],
        lambda ref, at: ref.at[pl.ds(*ROW_CUTS[at]), :],
        psend,
        precv,
        share_with_partner(proj_slot, core, qsend, qrecv, shared, awaited),
    )
    next(weights)
    loads[0].wait()

    @pl.loop(0, 4)
    def _(n):
        rows = pl.ds(pl.multiple_of(n * 256, 256), 256)
        some = patches[pl.ds(n * 4, 4)].reshape(256, 1280)
        for which in range(3):
            qkv[which, rows, :] = lax.dot_general(
                some, wq[which], (((1,), (1,)), ((), ())), preferred_element_type=jnp.float32
            ).astype(jnp.bfloat16)

    next(weights)
    end = ends[0:1, 0:1]

    def attend_rows(n):
        rows = pl.ds(pl.multiple_of(n * 256, 256), 256)
        scores = lax.dot_general(
            qkv[0, rows, :], qkv[1], (((1,), (1,)), ((), ())), preferred_element_type=jnp.float32
        ) * HD ** (-0.5)
        query_first = n * 256 + lax.broadcasted_iota(jnp.int32, (256, 1), 0) < end
        key_first = lax.broadcasted_iota(jnp.int32, (1, 1024), 1) < end
        query_first = jnp.where(query_first, 1, 0)
        key_first = jnp.where(key_first, 1, 0)
        scores = jnp.where(query_first == key_first, scores, -1e30)
        top = jnp.max(scores, axis=-1, keepdims=True)
        expo = jnp.exp(scores - top)
        share = (expo / jnp.sum(expo, axis=-1, keepdims=True)).astype(jnp.bfloat16)
        mixed = jnp.dot(share, qkv[2], preferred_element_type=jnp.float32).astype(jnp.bfloat16)
        att[pl.ds(n * 4, 4)] = mixed.reshape(4, 64, 128)

    for n in range(2):
        @pl.loop(2 * n, 2 * n + 2)
        def _(at):
            attend_rows(at)

        next(weights)
    sent = []
    for at, offset in enumerate(others):
        copy = remote(att.at[peer_index(*offset)], heads.at[me], hsend.at[at], hrecv.at[at], peer(*offset))
        copy.start()
        sent.append(copy)
    heads[me] = att[me]
    next(weights)
    run(weights)
    for copy in shared:
        copy.wait_send()
    for copy in awaited:
        copy.wait_recv()
    for at, (dy, dz) in enumerate(others):
        landing = heads.at[peer_index(4 - dy, 4 - dz)]
        remote(landing, landing, hsend.at[at], hrecv.at[at], peer(dy, dz)).wait_recv()
    for copy in sent:
        copy.wait_send()
    lined[...] = vit[...].astype(jnp.float32)

    @pl.loop(0, 16)
    def _(head):
        lined[...] += jnp.dot(heads[head, :, :80], wp[head], preferred_element_type=jnp.float32)

    ready = norm_rows(lined[...], merger_gain[...])
    for tile in range(10):
        tiles[tile] = ready[:, tile * 128 : tile * 128 + 128]
    for at in range(4):
        for tile in range(10):
            strided = tiles[tile, pl.ds(at, 16, stride=4), :]
            block_in[:, pl.ds(at * 1280 + tile * 128, 128)] = strided.astype(jnp.bfloat16)
    merged[pl.ds(pl.multiple_of(me * 16, 16), 16), :] = block_in[...]
    run(gather_plane(
        block_in,
        lambda t: merged.at[pl.ds(pl.multiple_of(t * 16, 16), 16), :],
        lambda ref, half: ref.at[:, pl.ds(half * 2560, 2560)],
        lambda ref, at: ref.at[:, pl.ds(at * 1280, 1280)],
        msend,
        mrecv,
    ))
    loads[2].wait()
    total = lax.dot_general(
        merged[...], one[...], (((1,), (1,)), ((), ())), preferred_element_type=jnp.float32
    )
    expanded[...] = (0.5 * total * (1.0 + lax.erf(total * (0.5 ** 0.5)))).astype(jnp.bfloat16)
    loads[3].wait()

    @pl.loop(0, 16)
    def _(n):
        columns = pl.ds(pl.multiple_of(n * 512, 512), 512)
        terms[:, columns] = jnp.dot(
            expanded[...], two[:, columns], preferred_element_type=jnp.float32
        ).astype(jnp.bfloat16)

    def emit(at, value):
        parcels[at, :, :2048] = value.astype(jnp.bfloat16)

    def term(t, at):
        return terms.at[pl.ds(pl.multiple_of(t * 16, 16), 16), pl.ds(at * 2048, 2048)]

    run(reduce_plane(term, got, made, sums, send, recv, emit))
    squares = jnp.zeros((16, 1), jnp.float32)
    for at in range(4):
        values = parcels[at, :, :2048].astype(jnp.float32)
        squares = squares + jnp.sum(values * values, axis=1, keepdims=True)
    high = squares.astype(jnp.bfloat16).astype(jnp.float32)
    low = squares - high
    lane = lax.broadcasted_iota(jnp.int32, (16, 128), 1)
    tail = jnp.where(lane == 0, high, jnp.where(lane == 1, low, 0.0)).astype(jnp.bfloat16)
    for at in range(4):
        parcels[at, :, 2048:] = tail
    mine = pl.ds(pl.multiple_of(x * 16, 16), 16)
    sent = []
    for step in (2, 1, 3):
        copy = remote(
            parcels.at[lax.rem(x + step, 4)], block.at[mine, :], xsend.at[step], xrecv.at[step], along_x(step)
        )
        copy.start()
        sent.append(copy)
    block[mine, :] = parcels[x]
    for step in (1, 3, 2):
        rows = pl.ds(pl.multiple_of(lax.rem(x + 4 - step, 4) * 16, 16), 16)
        landing = block.at[rows, :]
        remote(landing, landing, xsend.at[step], xrecv.at[step], along_x(step)).wait_recv()
    for copy in sent:
        copy.wait_send()
    forwarded, expected = [], []
    own_copy = remote(block, out.at[core, me], dsend.at[40], drecv.at[40], partner())
    own_copy.start()
    out[core, me] = block[...]
    run(gather_plane(
        block,
        lambda t: out.at[core, t],
        rows_half,
        rows_quarter,
        gsend,
        grecv,
        share_with_partner(lambda side, t: out.at[side, t], core, dsend, drecv, forwarded, expected),
    ))
    other = out.at[1 - core, me]
    expected.append(remote(other, other, dsend.at[40], drecv.at[40], partner()))
    own_copy.wait_send()
    for copy in forwarded:
        copy.wait_send()
    for copy in expected:
        copy.wait_recv()


def vision(vit, ends, ln_gain, merger_gain, w_qkv, w_proj, w_one, w_two, collective_id):
    anywhere = pl.BlockSpec(memory_space=pl.ANY)
    vmem = pl.BlockSpec(memory_space=pltpu.VMEM)
    dma = pltpu.SemaphoreType.DMA
    bf16 = jnp.bfloat16
    return pl.pallas_call(
        vision_kernel,
        out_shape=jax.ShapeDtypeStruct((2, 16, 64, WIDE), bf16),
        in_specs=[vmem] * 4 + [anywhere] * 4,
        out_specs=vmem,
        scratch_shapes=[
            pltpu.VMEM((64, 1280), bf16),
            pltpu.VMEM((16, 64, 1280), bf16),
            pltpu.VMEM((3, 1024, 128), bf16),
            pltpu.VMEM((3, 128, 1280), bf16),
            pltpu.VMEM((16, 80, 1280), bf16),
            pltpu.VMEM((16, 64, 128), bf16),
            pltpu.VMEM((16, 64, 128), bf16),
            pltpu.VMEM((64, 1280), jnp.float32),
            pltpu.VMEM((10, 64, 128), jnp.float32),
            pltpu.VMEM((16, 5120), bf16),
            pltpu.VMEM((256, 5120), bf16),
            pltpu.VMEM((320, 5120), bf16),
            pltpu.VMEM((256, 320), bf16),
            pltpu.VMEM((320, 8192), bf16),
            pltpu.VMEM((256, 8192), bf16),
            pltpu.VMEM((60, 16, 2048), bf16),
            pltpu.VMEM((20, 16, 2048), bf16),
            pltpu.VMEM((16, 16, 2048), bf16),
            pltpu.VMEM((4, 16, WIDE), bf16),
            pltpu.VMEM((64, WIDE), bf16),
            dma((4,)),
            dma((40,)), dma((40,)),
            dma((40,)), dma((40,)),
            dma((40,)), dma((40,)),
            dma((15,)), dma((15,)),
            dma((40,)), dma((40,)),
            dma((60,)), dma((60,)),
            dma((4,)), dma((4,)),
            dma((40,)), dma((40,)),
            dma((41,)), dma((41,)),
        ],
        compiler_params=pltpu.CompilerParams(
            collective_id=collective_id, has_side_effects=True, vmem_limit_bytes=56 * 1024 * 1024
        ),
        name="vision",
    )(vit, ends, ln_gain, merger_gain, w_qkv, w_proj, w_one, w_two)


GROUPS = ((0, 1024), (1024, 896))
BLOCKS = (((0, 0), (0, 1)), ((1, 1), (3, 0)), ((2, 0), (2, 1)), ((1, 0), (3, 1)))


def feed_forward_kernel(
    everyone, slots, gain, w_own, w_other, d_own, d_other, out,
    weights, downs, picks, raw, rows, strip, parts, came, hidden, got, made, sums, fin,
    wsem, osem, psend, precv, hsend, hrecv, send, recv, fsend, frecv,
):
    seq = lax.axis_index("seq")
    x, core = seq // 2, lax.rem(seq, 2)
    me = lax.axis_index("tp_0") * 4 + lax.axis_index("tp_1")
    real = w_own.shape[1]
    weights[:, pl.ds(1840, 80), :] = jnp.zeros((2, 80, 2048), jnp.bfloat16)
    downs[pl.ds(1840, 80), :] = jnp.zeros((80, 2048), jnp.bfloat16)
    sides = ((w_own, d_own, core), (w_other, d_other, 1 - core))

    def weight_copies(n):
        size = 256 if n < 7 else real - 1792
        return [
            pltpu.make_async_copy(
                w.at[:, pl.ds(n * 256, size), :],
                weights.at[:, pl.ds(n * 256, size), pl.ds(pl.multiple_of(at * 1024, 1024), 1024)],
                wsem.at[n, side],
            )
            for side, (w, _, at) in enumerate(sides)
        ]

    def down_copies():
        return [
            pltpu.make_async_copy(
                d, downs.at[pl.ds(0, real), pl.ds(pl.multiple_of(at * 1024, 1024), 1024)], osem.at[side]
            )
            for side, (_, d, at) in enumerate(sides)
        ]

    for n in range(8):
        for copy in weight_copies(n):
            copy.start()
    for copy in down_copies():
        copy.start()
    strip[...] = jnp.zeros_like(strip)

    def owner(step):
        return lax.rem(x + step, 4)

    def pick(block):
        upper, lower = BLOCKS[block]
        row = lax.broadcasted_iota(jnp.int32, (256, 1), 0)
        top = row < 128
        at = jnp.where(top, owner(upper[0]), owner(lower[0]))
        row = jnp.where(top, row + upper[1] * 128, row - 128 + lower[1] * 128)
        slot = (row // 16) * 128 + core * 64 + at * 16 + row % 16
        picks[...] = jnp.where(slots[...] == slot, 1.0, 0.0).astype(jnp.bfloat16)

        def piece(begin, size):
            value = jnp.dot(picks[...], everyone[:, pl.ds(begin, size)], preferred_element_type=jnp.float32)
            raw[:, pl.ds(begin, size)] = value.astype(jnp.bfloat16)

        @pl.loop(0, 8)
        def _(n):
            piece(pl.multiple_of(n * 256, 256), 256)

        piece(2048, 128)
        square = raw[:, 2048:2049].astype(jnp.float32) + raw[:, 2049:2050].astype(jnp.float32)
        inverse = lax.rsqrt(square / D + 1e-06)
        rows[...] = (raw[:, :2048].astype(jnp.float32) * inverse * gain[...]).astype(jnp.bfloat16)
        for base, (step, half) in zip((0, 128), (upper, lower)):
            found = raw[pl.ds(pl.multiple_of(base + lax.rem(me, 8) * 16, 16), 16), :2048]
            here = me // 8 == half
            strip[step] = jnp.where(here, found, strip[step])

    def multiply(step, group, first=False):
        def piece(begin, size):
            for half in range(2):
                value = lax.dot_general(
                    rows[...], weights[half, pl.ds(begin, size), :], (((1,), (1,)), ((), ())),
                    preferred_element_type=jnp.float32,
                )
                parts[step, half, :, pl.ds(begin, size)] = value.astype(jnp.bfloat16)

        if first:
            for n in range(4 * group, 4 * group + 4):
                for copy in weight_copies(n):
                    copy.wait()
        full = 4 if group == 0 else 3

        @pl.loop(0, full)
        def _(n):
            piece(pl.multiple_of(GROUPS[group][0] + n * 256, 256), 256)

        if group == 1:
            piece(1792, 128)

    def cut(ref, sub):
        begin, size = GROUPS[sub % 2]
        return ref.at[:, pl.ds(sub // 2 * 128, 128), pl.ds(begin, size)]

    sent = []

    def part_slot(kind, index):
        return came.at[kind * 2 + index, :, :, pl.ds(0, GROUPS[index][1])]

    part_sends = {}

    def pass_part(kind, index, src, way, step):
        at = kind * 2 + index
        copy = remote(src, part_slot(kind, index), psend.at[at], precv.at[at], along_x(way))
        copy.start()
        part_sends.setdefault(step, []).append(copy)

    def part_landed(kind, index):
        at = kind * 2 + index
        landing = part_slot(kind, index)
        remote(landing, landing, psend.at[at], precv.at[at], along_x(1)).wait_recv()
        return landing

    pick(2)
    for index in range(2):
        multiply(2, index, True)
        if index == 0:
            greet(plane_neighbours() + [along_x(step) for step in (1, 3)] + [partner()])
        pass_part(0, index, cut(parts.at[2], index), 1, 2)
        pass_part(3, index, cut(parts.at[2], 2 + index), 3, 2)
    pick(1)
    for index in range(2):
        multiply(1, index)
        pass_part(1, index, cut(parts.at[1], index), 1, 1)
        pass_part(4, index, cut(parts.at[1], 2 + index), 3, 1)
    pick(3)
    for index in range(2):
        multiply(3, index)
        for kind, sub, way in ((0, index, 1), (3, 2 + index, 3)):
            arrived = part_landed(kind, index)
            target = cut(parts.at[3], sub)
            target[...] = (target[...].astype(jnp.float32) + arrived[...].astype(jnp.float32)).astype(jnp.bfloat16)
            pass_part(kind + 2, index, target, way, 3)
    pick(0)
    for index in range(2):
        multiply(0, index)

    def hidden_piece(step, sub):
        begin, size = GROUPS[sub % 2]
        return hidden.at[owner(step), pl.ds(sub // 2 * 128, 128), pl.ds(begin, size)]

    def pass_hidden(at, piece, step):
        copy = remote(piece, piece, hsend.at[at], hrecv.at[at], along_x(step))
        copy.start()
        sent.append(copy)

    def hidden_landed(at, piece):
        remote(piece, piece, hsend.at[at], hrecv.at[at], along_x(1)).wait_recv()

    for index in range(2):
        for sub, near, far in ((index, 4, 2), (2 + index, 1, 5)):
            one = part_landed(near, index)
            two = part_landed(far, index)
            own = cut(parts.at[0], sub)
            gate, up = [
                own[half].astype(jnp.float32) + one[half].astype(jnp.float32) + two[half].astype(jnp.float32)
                for half in range(2)
            ]
            piece = hidden_piece(0, sub)
            piece[...] = (gate / (1.0 + jnp.exp(-gate)) * up).astype(jnp.bfloat16)
            pass_hidden(sub, piece, 1)
            pass_hidden(4 + sub, piece, 3)
    for copy in down_copies():
        copy.wait()

    def project(step):
        at = owner(step)
        for copy in part_sends.get(step, []):
            copy.wait_send()
        for side in range(2):
            @pl.loop(0, 4)
            def _(n):
                begin = pl.multiple_of(n * 256, 256)
                value = jnp.dot(
                    hidden[at],
                    downs[:, pl.ds(pl.multiple_of(side * 1024 + begin, 256), 256)],
                    preferred_element_type=jnp.float32,
                )
                parts[step, side, :, pl.ds(begin, 256)] = value.astype(jnp.bfloat16)

    def reduction(step):
        def term(t, at):
            return parts.at[step, at // 2, pl.ds(pl.multiple_of(t * 16, 16), 16), pl.ds(at % 2 * 512, 512)]

        def emit(at, value):
            total = value + strip[step, :, pl.ds(at * 512, 512)].astype(jnp.float32)
            target = pl.ds(pl.multiple_of(owner(step) * 16, 16), 16)
            fin[at // 2, target, pl.ds(at % 2 * 512, 512)] = total.astype(jnp.bfloat16)

        return reduce_plane(
            term, got.at[step], made.at[step], sums.at[step], send.at[step], recv.at[step], emit, False
        )

    def relay(index):
        hidden_landed(index, hidden_piece(3, index))
        pass_hidden(8 + index, hidden_piece(3, index), 1)
        hidden_landed(4 + 2 + index, hidden_piece(1, 2 + index))
        pass_hidden(10 + index, hidden_piece(1, 2 + index), 3)

    flows = {step: reduction(step) for step in range(4)}
    project(0)
    next(flows[0])
    relay(0)
    next(flows[0])
    relay(1)
    next(flows[0])
    for index in range(2):
        hidden_landed(2 + index, hidden_piece(3, 2 + index))
    project(3)
    next(flows[3])
    for index in range(2):
        hidden_landed(4 + index, hidden_piece(1, index))
    project(1)
    next(flows[1])
    next(flows[0])
    next(flows[3])
    next(flows[1])
    for index in range(2):
        hidden_landed(8 + index, hidden_piece(2, index))
        hidden_landed(10 + index, hidden_piece(2, 2 + index))
    project(2)
    next(flows[2])
    next(flows[3])
    next(flows[1])
    next(flows[2])
    next(flows[3])
    next(flows[1])
    next(flows[2])
    run(flows[0])
    run(flows[3])
    run(flows[1])
    run(flows[2])
    mine = pl.ds(pl.multiple_of(core * 64, 64), 64)
    theirs = pl.ds(pl.multiple_of((1 - core) * 64, 64), 64)
    swap = remote(fin.at[1 - core], out.at[mine, :], fsend, frecv, partner())
    swap.start()
    out[mine, :] = fin[core]
    swap.wait_send()
    landing = out.at[theirs, :]
    remote(landing, landing, fsend, frecv, partner()).wait_recv()
    for copy in sent + part_sends.get(0, []):
        copy.wait_send()


def feed_forward(everyone, slots, gain, w_own, w_other, d_own, d_other, collective_id):
    anywhere = pl.BlockSpec(memory_space=pl.ANY)
    vmem = pl.BlockSpec(memory_space=pltpu.VMEM)
    dma = pltpu.SemaphoreType.DMA
    bf16 = jnp.bfloat16
    return pl.pallas_call(
        feed_forward_kernel,
        out_shape=jax.ShapeDtypeStruct((128, 1024), bf16),
        in_specs=[vmem, vmem, vmem, anywhere, anywhere, anywhere, anywhere],
        out_specs=vmem,
        scratch_shapes=[
            pltpu.VMEM((2, PADDED, 2048), bf16),
            pltpu.VMEM((PADDED, 2048), bf16),
            pltpu.VMEM((256, 2048), bf16),
            pltpu.VMEM((256, WIDE), bf16),
            pltpu.VMEM((256, 2048), bf16),
            pltpu.VMEM((4, 16, 2048), bf16),
            pltpu.VMEM((4, 2, 256, PADDED), bf16),
            pltpu.VMEM((12, 2, 128, 1024), bf16),
            pltpu.VMEM((4, 256, PADDED), bf16),
            pltpu.VMEM((4, 60, 16, 512), bf16),
            pltpu.VMEM((4, 20, 16, 512), bf16),
            pltpu.VMEM((4, 16, 16, 512), bf16),
            pltpu.VMEM((2, 64, 1024), bf16),
            dma((8, 2)),
            dma((2,)),
            dma((12,)),
            dma((12,)),
            dma((12,)),
            dma((12,)),
            dma((4, 60)),
            dma((4, 60)),
            dma,
            dma,
        ],
        compiler_params=pltpu.CompilerParams(
            collective_id=collective_id, has_side_effects=True, vmem_limit_bytes=67043328
        ),
        name="feed_forward",
    )(everyone, slots, gain, w_own, w_other, d_own, d_other)


def local(
    vit_input,
    image_lengths,
    positions,
    vit_ln_gain,
    w_qkv,
    w_proj,
    merger_ln_gain,
    merger_w1,
    merger_w2,
    norm_gain,
    gate_up_weight,
    down_weight,
):
    seq_size = lax.axis_size("seq")
    core = lax.rem(lax.axis_index("seq"), 2)
    swap = [(i, i ^ 1) for i in range(seq_size)]
    gate_up_rows = jnp.transpose(gate_up_weight, (1, 2, 0))
    other_rows = lax.ppermute(gate_up_rows, "seq", swap)
    other_down = lax.ppermute(down_weight, "seq", swap)
    other_gain = lax.ppermute(norm_gain, "seq", swap)
    everyone = vision(
        vit_input,
        jnp.broadcast_to(image_lengths[0, 0] * 4, (8, 128)),
        vit_ln_gain[None],
        merger_ln_gain[None],
        jnp.transpose(w_qkv, (1, 2, 0)),
        w_proj,
        jnp.transpose(merger_w1),
        merger_w2,
        1,
    ).reshape(-1, WIDE)
    slots = positions.reshape(4, 2, 16, 16).transpose(1, 2, 0, 3).reshape(1, -1)
    gain = jnp.where(
        core == 0, jnp.concatenate([norm_gain, other_gain]), jnp.concatenate([other_gain, norm_gain])
    )
    return feed_forward(
        everyone, slots, gain[None], gate_up_rows, other_rows, down_weight, other_down, 2
    )


def solution(mesh):
    finer = Mesh(mesh.devices.reshape(mesh.shape["seq"], 4, 4), ("seq", "tp_0", "tp_1"))
    in_specs = (
        P(SEQ_TP, None),
        P("seq", None),
        P(),
        P(),
        P(None, None, TP),
        P(TP, None),
        P(),
        P(None, TP),
        P(TP, None),
        P("seq"),
        P("seq", None, TP),
        P(TP, "seq"),
    )
    out_specs = P(TP, "seq")
    return jax.shard_map(local, mesh=finer, in_specs=in_specs, out_specs=out_specs, check_vma=False)
```

```python
import jax
import jax.numpy as jnp
from jax import lax
from jax.experimental import pallas as pl
from jax.experimental.pallas import tpu as pltpu
from jax.sharding import Mesh
from jax.sharding import PartitionSpec as P

D = 8192
HD = 80
TP = ("tp_0", "tp_1")
SEQ_TP = ("seq", "tp_0", "tp_1")

MESH_ID = pl.DeviceIdType.MESH
AXES = ("tp_0", "tp_1")


def ring(axis, step):
    return {axis: lax.rem(lax.axis_index(axis) + step, 4)}


def remote(src, dst, send, recv, target):
    return pltpu.make_async_remote_copy(
        src_ref=src, dst_ref=dst, send_sem=send, recv_sem=recv, device_id=target, device_id_type=MESH_ID
    )


def greet(targets):
    barrier = pltpu.get_barrier_semaphore()
    for target in targets:
        pl.semaphore_signal(barrier, inc=1, device_id=target, device_id_type=MESH_ID)
    pl.semaphore_wait(barrier, len(targets))


def plane_neighbours():
    return [ring(axis, step) for axis in AXES for step in (1, 3)]


def gather_plane(own, slot, half_cut, quarter_cut, send, recv, forward=None):
    here = [lax.axis_index(axis) for axis in AXES]
    sent = []

    def index(half, first, second):
        offsets = (first, second) if half == 0 else (second, first)
        spots = [lax.rem(at + off, 4) for at, off in zip(here, offsets)]
        return spots[0] * 4 + spots[1]

    def place(half, first, second):
        return slot(index(half, first, second))

    def source(half, first, second):
        return own if (first, second) == (0, 0) else place(half, first, second)

    def start(half, phase, kind, axis, step, first, second, cut):
        at = half * 20 + phase * 4 + kind
        copy = remote(
            cut(source(half, first, second)), cut(place(half, first, second)), send.at[at], recv.at[at], ring(axis, step)
        )
        copy.start()
        sent.append(copy)

    def landed(half, phase, kind, axis, first, second, cut):
        at = half * 20 + phase * 4 + kind
        target = cut(place(half, first, second))
        remote(target, target, send.at[at], recv.at[at], ring(axis, 1)).wait_recv()
        if forward is not None:
            forward(at, lambda base: cut(base(index(half, first, second))))

    def axes(half):
        return (AXES[0], AXES[1]) if half == 0 else (AXES[1], AXES[0])

    def cuts(half):
        return (
            lambda ref: half_cut(ref, half),
            lambda ref: quarter_cut(ref, 2 * half),
            lambda ref: quarter_cut(ref, 2 * half + 1),
        )

    def spread(half, phase, first):
        whole, _, _ = cuts(half)
        axis = axes(half)[1]
        start(half, phase, 0, axis, 1, first, 0, whole)
        start(half, phase, 1, axis, 3, first, 0, whole)

    def relay(half, phase, first):
        whole, low, high = cuts(half)
        axis = axes(half)[1]
        landed(half, phase, 0, axis, first, 3, whole)
        start(half, phase, 2, axis, 1, first, 3, low)
        landed(half, phase, 1, axis, first, 1, whole)
        start(half, phase, 3, axis, 3, first, 1, high)

    def finish(half, phase, first):
        whole, low, high = cuts(half)
        axis = axes(half)[1]
        landed(half, phase, 2, axis, first, 2, low)
        landed(half, phase, 3, axis, first, 2, high)

    for half in (0, 1):
        whole, _, _ = cuts(half)
        start(half, 0, 0, axes(half)[0], 1, 0, 0, whole)
        start(half, 0, 1, axes(half)[0], 3, 0, 0, whole)
    for half in (0, 1):
        spread(half, 1, 0)
    yield
    for half in (0, 1):
        whole, low, high = cuts(half)
        axis = axes(half)[0]
        landed(half, 0, 0, axis, 3, 0, whole)
        start(half, 0, 2, axis, 1, 3, 0, low)
        spread(half, 2, 3)
        landed(half, 0, 1, axis, 1, 0, whole)
        start(half, 0, 3, axis, 3, 1, 0, high)
        spread(half, 3, 1)
    yield
    for half in (0, 1):
        relay(half, 1, 0)
    yield
    for half in (0, 1):
        whole, low, high = cuts(half)
        axis = axes(half)[0]
        landed(half, 0, 2, axis, 2, 0, low)
        landed(half, 0, 3, axis, 2, 0, high)
        spread(half, 4, 2)
    yield
    for phase, first in ((2, 3), (3, 1), (4, 2)):
        for half in (0, 1):
            relay(half, phase, first)
    yield
    for phase, first in ((1, 0), (2, 3), (3, 1), (4, 2)):
        for half in (0, 1):
            finish(half, phase, first)
    for copy in sent:
        copy.wait_send()


def reduce_plane(term, got, made, sums, send, recv, emit, eager=True):
    here = [lax.axis_index(axis) for axis in AXES]
    sent = []

    def axes(half):
        return (AXES[1], AXES[0]) if half == 0 else (AXES[0], AXES[1])

    def part(half, first, second, which):
        offsets = (first, second) if half == 0 else (second, first)
        spots = [lax.rem(at + off, 4) for at, off in zip(here, offsets)]
        return term(spots[0] * 4 + spots[1], 2 * half + which)

    def phase_source(half, phase):
        if phase < 4:
            return lambda offset, which: part(half, phase, offset, which)
        return lambda offset, which: sums.at[half * 8 + offset * 2 + which]

    def slot(half, phase, kind):
        return half * 30 + phase * 6 + kind

    def start(half, phase, kind, src, step):
        axis = axes(half)[0 if phase < 4 else 1]
        at = slot(half, phase, kind)
        copy = remote(src, got.at[at], send.at[at], recv.at[at], ring(axis, step))
        copy.start()
        sent.append(copy)

    def landed(half, phase, kind):
        at = slot(half, phase, kind)
        axis = axes(half)[0 if phase < 4 else 1]
        remote(got.at[at], got.at[at], send.at[at], recv.at[at], ring(axis, 1)).wait_recv()
        return got[at].astype(jnp.float32)

    def raw(half, phase):
        own = phase_source(half, phase)
        start(half, phase, 0, own(2, 0), 1)
        start(half, phase, 3, own(2, 1), 3)
        start(half, phase, 1, own(1, 1), 1)
        start(half, phase, 4, own(3, 0), 3)

    def summed(half, phase):
        own = phase_source(half, phase)
        for kind, offset, which, step in ((0, 1, 0, 1), (3, 3, 1, 3)):
            at = half * 10 + phase * 2 + which
            made[at] = (own(offset, which)[...].astype(jnp.float32) + landed(half, phase, kind)).astype(made.dtype)
            start(half, phase, kind + 2, made.at[at], step)

    def total(half, phase):
        own = phase_source(half, phase)
        return [
            own(0, which)[...].astype(jnp.float32) + landed(half, phase, near) + landed(half, phase, far)
            for which, near, far in ((0, 4, 2), (1, 1, 5))
        ]

    def settle(half, phase):
        for which, value in enumerate(total(half, phase)):
            sums[half * 8 + phase * 2 + which] = value.astype(sums.dtype)

    order = (2, 1, 3, 0)
    both = (0, 1)

    def late(first):
        own = phase_source_of_last
        for half in both:
            source = own(half)
            if first == 2:
                start(half, 4, 0, source(2, 0), 1)
                start(half, 4, 3, source(2, 1), 3)
            if first == 1:
                start(half, 4, 1, source(1, 1), 1)
            if first == 3:
                start(half, 4, 4, source(3, 0), 3)

    def phase_source_of_last(half):
        return phase_source(half, 4)

    for half in both:
        for phase in order[:2] if eager else order:
            raw(half, phase)
        yield
    for at, phase in enumerate(order):
        for half in both:
            summed(half, phase)
        if eager and at + 2 < 4:
            for half in both:
                raw(half, order[at + 2])
        if eager and at >= 1:
            for half in both:
                settle(half, order[at - 1])
            late(order[at - 1])
    yield
    if not eager:
        for phase in order[:3]:
            for half in both:
                settle(half, phase)
            late(phase)
    yield
    for half in both:
        summed(half, 4)
    yield
    for half in both:
        settle(half, 0)
    for half in both:
        for which, value in enumerate(total(half, 4)):
            emit(2 * half + which, value)
    for copy in sent:
        copy.wait_send()


def run(steps):
    for _ in steps:
        pass
WIDE = 2176
PADDED = 1920


def along_x(step):
    seq = lax.axis_index("seq")
    return {"seq": lax.rem(seq + 2 * step, 8)}


def partner():
    seq = lax.axis_index("seq")
    return {"seq": seq + 1 - 2 * lax.rem(seq, 2)}


ROW_CUTS = ((0, 32), (32, 16), (48, 16), (64, 16))
ROW_HALVES = ((0, 48), (48, 32))


def share_with_partner(buffer, core, send, recv, sent, expected):
    def forward(at, view):
        piece = view(lambda t: buffer(core, t))
        copy = remote(piece, piece, send.at[at], recv.at[at], partner())
        copy.start()
        sent.append(copy)
        other = view(lambda t: buffer(1 - core, t))
        expected.append(remote(other, other, send.at[at], recv.at[at], partner()))

    return forward


def norm_rows(values, gain):
    mean = jnp.mean(values, axis=-1, keepdims=True)
    centered = values - mean
    variance = jnp.mean(centered * centered, axis=-1, keepdims=True)
    return centered * lax.rsqrt(variance + 1e-06) * gain


def vision_kernel(
    vit, ends, ln_gain, merger_gain, w_qkv, w_proj, w_one, w_two, out,
    own, patches, qkv, wq, wp, att, heads, lined, tiles, block_in, merged, one, expanded, two, terms,
    got, made, sums, parcels, block, held,
    wsem, osem, asend, arecv, psend, precv, qsend, qrecv, hsend, hrecv, msend, mrecv,
    send, recv, xsend, xrecv, gsend, grecv, dsend, drecv,
):
    seq = lax.axis_index("seq")
    x, core = seq // 2, lax.rem(seq, 2)
    y, z = [lax.axis_index(axis) for axis in AXES]
    me = y * 4 + z
    others = [(dy, dz) for dy in range(4) for dz in range(4) if (dy, dz) != (0, 0)]

    def peer(dy, dz):
        return {"tp_0": lax.rem(y + dy, 4), "tp_1": lax.rem(z + dz, 4)}

    def peer_index(dy, dz):
        return lax.rem(y + dy, 4) * 4 + lax.rem(z + dz, 4)

    def proj_slot(side, t):
        return wp.at[t, :, pl.ds(pl.multiple_of(side * 640, 128), 640)]

    wq[:, pl.ds(80, 48), :] = jnp.zeros((3, 48, 1280), jnp.bfloat16)
    loads = [
        pltpu.make_async_copy(w_qkv, wq.at[:, pl.ds(0, 80), :], wsem.at[0]),
        pltpu.make_async_copy(w_proj, wp.at[me], wsem.at[1]),
        pltpu.make_async_copy(w_one, one, wsem.at[2]),
        pltpu.make_async_copy(w_two, two, wsem.at[3]),
    ]
    for copy in loads:
        copy.start()
    targets = [peer(*offset) for offset in others] + [along_x(step) for step in (1, 2, 3)] + [partner()]
    barrier = pltpu.get_barrier_semaphore()
    for target in targets:
        pl.semaphore_signal(barrier, inc=1, device_id=target, device_id_type=MESH_ID)
    own[...] = norm_rows(vit[...].astype(jnp.float32), ln_gain[...][None]).astype(jnp.bfloat16)
    pl.semaphore_wait(barrier, len(targets))

    rows_half = lambda ref, half: ref.at[pl.ds(half * 32, 32), :]
    rows_quarter = lambda ref, at: ref.at[pl.ds(at * 16, 16), :]
    patches[me] = own[...]
    arrive = gather_plane(own, lambda t: patches.at[t], rows_half, rows_quarter, asend, arecv)
    next(arrive)
    loads[1].wait()
    shared, awaited = [], []
    weights = gather_plane(
        proj_slot(core, me),
        lambda t: proj_slot(core, t),
        lambda ref, half: ref.at[pl.ds(*ROW_HALVES[half]), :],
        lambda ref, at: ref.at[pl.ds(*ROW_CUTS[at]), :],
        psend,
        precv,
        share_with_partner(proj_slot, core, qsend, qrecv, shared, awaited),
    )
    next(weights)
    next(arrive)
    next(arrive)
    next(arrive)
    next(weights)
    next(arrive)
    next(weights)
    run(arrive)
    loads[0].wait()

    @pl.loop(0, 4)
    def _(n):
        rows = pl.ds(pl.multiple_of(n * 256, 256), 256)
        some = patches[pl.ds(n * 4, 4)].reshape(256, 1280)
        for which in range(3):
            qkv[which, rows, :] = lax.dot_general(
                some, wq[which], (((1,), (1,)), ((), ())), preferred_element_type=jnp.float32
            ).astype(jnp.bfloat16)

    next(weights)
    end = ends[0:1, 0:1] * 4

    def attend_rows(n):
        rows = pl.ds(pl.multiple_of(n * 256, 256), 256)
        scores = lax.dot_general(
            qkv[0, rows, :], qkv[1], (((1,), (1,)), ((), ())), preferred_element_type=jnp.float32
        ) * HD ** (-0.5)
        query_first = n * 256 + lax.broadcasted_iota(jnp.int32, (256, 1), 0) < end
        key_first = lax.broadcasted_iota(jnp.int32, (1, 1024), 1) < end
        query_first = jnp.where(query_first, 1, 0)
        key_first = jnp.where(key_first, 1, 0)
        scores = jnp.where(query_first == key_first, scores, -1e30)
        top = jnp.max(scores, axis=-1, keepdims=True)
        expo = jnp.exp(scores - top)
        share = (expo / jnp.sum(expo, axis=-1, keepdims=True)).astype(jnp.bfloat16)
        mixed = jnp.dot(share, qkv[2], preferred_element_type=jnp.float32).astype(jnp.bfloat16)
        att[pl.ds(n * 4, 4)] = mixed.reshape(4, 64, 128)

    for n in range(2):
        @pl.loop(2 * n, 2 * n + 2)
        def _(at):
            attend_rows(at)

        if n == 0:
            next(weights)
    sent = []
    for at, offset in enumerate(others):
        copy = remote(att.at[peer_index(*offset)], heads.at[me], hsend.at[at], hrecv.at[at], peer(*offset))
        copy.start()
        sent.append(copy)
    heads[me] = att[me]
    run(weights)
    for copy in shared:
        copy.wait_send()
    for copy in awaited:
        copy.wait_recv()
    for at, (dy, dz) in enumerate(others):
        landing = heads.at[peer_index(4 - dy, 4 - dz)]
        remote(landing, landing, hsend.at[at], hrecv.at[at], peer(dy, dz)).wait_recv()
    for copy in sent:
        copy.wait_send()
    lined[...] = vit[...].astype(jnp.float32)

    @pl.loop(0, 16)
    def _(head):
        lined[...] += jnp.dot(heads[head, :, :80], wp[head], preferred_element_type=jnp.float32)

    ready = norm_rows(lined[...], merger_gain[...][None])
    for tile in range(10):
        tiles[tile] = ready[:, tile * 128 : tile * 128 + 128]
    for at in range(4):
        for tile in range(10):
            strided = tiles[tile, pl.ds(at, 16, stride=4), :]
            block_in[:, pl.ds(at * 1280 + tile * 128, 128)] = strided.astype(jnp.bfloat16)
    merged[pl.ds(pl.multiple_of(me * 16, 16), 16), :] = block_in[...]
    run(gather_plane(
        block_in,
        lambda t: merged.at[pl.ds(pl.multiple_of(t * 16, 16), 16), :],
        lambda ref, half: ref.at[:, pl.ds(half * 2560, 2560)],
        lambda ref, at: ref.at[:, pl.ds(at * 1280, 1280)],
        msend,
        mrecv,
    ))
    loads[2].wait()
    total = lax.dot_general(
        merged[...], one[...], (((1,), (1,)), ((), ())), preferred_element_type=jnp.float32
    )
    expanded[...] = (0.5 * total * (1.0 + lax.erf(total * (0.5 ** 0.5)))).astype(jnp.bfloat16)
    loads[3].wait()

    def share_of(half):
        @pl.loop(8 * half, 8 * half + 8)
        def _(n):
            columns = pl.ds(pl.multiple_of(n * 512, 512), 512)
            terms[:, columns] = jnp.dot(
                expanded[...], two[:, columns], preferred_element_type=jnp.float32
            ).astype(jnp.bfloat16)

    def emit(at, value):
        parcels[at, :, :2048] = value.astype(jnp.bfloat16)

    def term(t, at):
        return terms.at[pl.ds(pl.multiple_of(t * 16, 16), 16), pl.ds(at * 2048, 2048)]

    shares = reduce_plane(term, got, made, sums, send, recv, emit)
    share_of(0)
    next(shares)
    share_of(1)
    run(shares)
    squares = jnp.zeros((16, 1), jnp.float32)
    for at in range(4):
        values = parcels[at, :, :2048].astype(jnp.float32)
        squares = squares + jnp.sum(values * values, axis=1, keepdims=True)
    high = squares.astype(jnp.bfloat16).astype(jnp.float32)
    low = squares - high
    lane = lax.broadcasted_iota(jnp.int32, (16, 128), 1)
    tail = jnp.where(lane == 0, high, jnp.where(lane == 1, low, 0.0)).astype(jnp.bfloat16)
    for at in range(4):
        parcels[at, :, 2048:] = tail
    sent = []
    for step in (2, 1, 3):
        copy = remote(
            parcels.at[lax.rem(x + step, 4)], block.at[x], xsend.at[step], xrecv.at[step], along_x(step)
        )
        copy.start()
        sent.append(copy)
    block[x] = parcels[x]
    for step in (1, 3, 2):
        landing = block.at[lax.rem(x + 4 - step, 4)]
        remote(landing, landing, xsend.at[step], xrecv.at[step], along_x(step)).wait_recv()
    for copy in sent:
        copy.wait_send()
    forwarded, expected = [], []

    def spot(side, t):
        return held.at[:, side, t]

    own_copy = remote(block, spot(core, me), dsend.at[40], drecv.at[40], partner())
    own_copy.start()
    held[:, core, me] = block[...]
    run(gather_plane(
        block,
        lambda t: spot(core, t),
        lambda ref, half: ref.at[pl.ds(half * 2, 2)],
        lambda ref, at: ref.at[pl.ds(at, 1)],
        gsend,
        grecv,
        share_with_partner(spot, core, dsend, drecv, forwarded, expected),
    ))
    copies = [pltpu.make_async_copy(held.at[:, side], out.at[:, side], osem.at[at]) for at, side in enumerate((core, 1 - core))]
    copies[0].start()
    other = spot(1 - core, me)
    expected.append(remote(other, other, dsend.at[40], drecv.at[40], partner()))
    for copy in expected:
        copy.wait_recv()
    copies[1].start()
    own_copy.wait_send()
    for copy in forwarded:
        copy.wait_send()
    for copy in copies:
        copy.wait()


def vision(vit, ends, ln_gain, merger_gain, w_qkv, w_proj, w_one, w_two, collective_id):
    anywhere = pl.BlockSpec(memory_space=pl.ANY)
    vmem = pl.BlockSpec(memory_space=pltpu.VMEM)
    dma = pltpu.SemaphoreType.DMA
    bf16 = jnp.bfloat16
    return pl.pallas_call(
        vision_kernel,
        out_shape=jax.ShapeDtypeStruct((4, 2, 16, 16, WIDE), bf16),
        in_specs=[vmem] * 4 + [anywhere] * 4,
        out_specs=anywhere,
        scratch_shapes=[
            pltpu.VMEM((64, 1280), bf16),
            pltpu.VMEM((16, 64, 1280), bf16),
            pltpu.VMEM((3, 1024, 128), bf16),
            pltpu.VMEM((3, 128, 1280), bf16),
            pltpu.VMEM((16, 80, 1280), bf16),
            pltpu.VMEM((16, 64, 128), bf16),
            pltpu.VMEM((16, 64, 128), bf16),
            pltpu.VMEM((64, 1280), jnp.float32),
            pltpu.VMEM((10, 64, 128), jnp.float32),
            pltpu.VMEM((16, 5120), bf16),
            pltpu.VMEM((256, 5120), bf16),
            pltpu.VMEM((320, 5120), bf16),
            pltpu.VMEM((256, 320), bf16),
            pltpu.VMEM((320, 8192), bf16),
            pltpu.VMEM((256, 8192), bf16),
            pltpu.VMEM((60, 16, 2048), bf16),
            pltpu.VMEM((20, 16, 2048), bf16),
            pltpu.VMEM((16, 16, 2048), bf16),
            pltpu.VMEM((4, 16, WIDE), bf16),
            pltpu.VMEM((4, 16, WIDE), bf16),
            pltpu.VMEM((4, 2, 16, 16, WIDE), bf16),
            dma((4,)),
            dma((2,)),
            dma((40,)), dma((40,)),
            dma((40,)), dma((40,)),
            dma((40,)), dma((40,)),
            dma((15,)), dma((15,)),
            dma((40,)), dma((40,)),
            dma((60,)), dma((60,)),
            dma((4,)), dma((4,)),
            dma((40,)), dma((40,)),
            dma((41,)), dma((41,)),
        ],
        compiler_params=pltpu.CompilerParams(
            collective_id=collective_id, has_side_effects=True, vmem_limit_bytes=56 * 1024 * 1024
        ),
        name="vision",
    )(vit, ends, ln_gain, merger_gain, w_qkv, w_proj, w_one, w_two)


GROUPS = ((0, 512), (512, 1408))
BLOCKS = (((0, 0), (0, 1)), ((1, 1), (3, 0)), ((2, 0), (2, 1)), ((1, 0), (3, 1)))


def feed_forward_kernel(
    tokens, slots, own_gain, other_gain, w_own, w_other, d_own, d_other, out,
    weights, downs, everyone, gain, picks, raw, rows, strip, parts, came_first, came_second, hidden, got, made, sums, fin,
    esem, wsem, osem, psend, precv, hsend, hrecv, send, recv, fsend, frecv,
):
    seq = lax.axis_index("seq")
    x, core = seq // 2, lax.rem(seq, 2)
    me = lax.axis_index("tp_0") * 4 + lax.axis_index("tp_1")
    real = w_own.shape[1]
    wide = [(n * 256, 256 if n < 8 else 128) for n in range(9)]
    entering = [
        pltpu.make_async_copy(tokens.at[:, pl.ds(*cut)], everyone.at[:, pl.ds(*cut)], esem.at[n])
        for n, cut in enumerate(wide)
    ]
    for copy in entering:
        copy.start()
    first_core = core == 0
    gain[:, :1024] = jnp.where(first_core, own_gain[...], other_gain[...])[None]
    gain[:, 1024:] = jnp.where(first_core, other_gain[...], own_gain[...])[None]
    weights[:, pl.ds(1840, 80), :] = jnp.zeros((2, 80, 2048), jnp.bfloat16)
    downs[pl.ds(1840, 80), :] = jnp.zeros((80, 2048), jnp.bfloat16)
    sides = ((w_own, d_own, core), (w_other, d_other, 1 - core))

    def weight_copies(n):
        size = 256 if n < 7 else real - 1792
        return [
            pltpu.make_async_copy(
                w.at[:, pl.ds(n * 256, size), :],
                weights.at[:, pl.ds(n * 256, size), pl.ds(pl.multiple_of(at * 1024, 1024), 1024)],
                wsem.at[n, side],
            )
            for side, (w, _, at) in enumerate(sides)
        ]

    def down_copies():
        return [
            pltpu.make_async_copy(
                d, downs.at[pl.ds(0, real), pl.ds(pl.multiple_of(at * 1024, 1024), 1024)], osem.at[side]
            )
            for side, (_, d, at) in enumerate(sides)
        ]

    for n in range(8):
        for copy in weight_copies(n):
            copy.start()
    for copy in down_copies():
        copy.start()
    strip[...] = jnp.zeros_like(strip)

    def owner(step):
        return lax.rem(x + step, 4)

    def pick(block, first=False):
        upper, lower = BLOCKS[block]
        row = lax.broadcasted_iota(jnp.int32, (256, 1), 0)
        top = row < 128
        at = jnp.where(top, owner(upper[0]), owner(lower[0]))
        row = jnp.where(top, row + upper[1] * 128, row - 128 + lower[1] * 128)
        slot = (row // 16) * 128 + core * 64 + at * 16 + row % 16
        picks[...] = jnp.where(slots[...][None] == slot, 1.0, 0.0).astype(jnp.bfloat16)

        def piece(begin, size):
            value = jnp.dot(picks[...], everyone[:, pl.ds(begin, size)], preferred_element_type=jnp.float32)
            raw[:, pl.ds(begin, size)] = value.astype(jnp.bfloat16)

        if first:
            for n, cut in enumerate(wide):
                entering[n].wait()
                piece(*cut)
        else:
            @pl.loop(0, 8)
            def _(n):
                piece(pl.multiple_of(n * 256, 256), 256)

            piece(2048, 128)
        square = raw[:, 2048:2049].astype(jnp.float32) + raw[:, 2049:2050].astype(jnp.float32)
        inverse = lax.rsqrt(square / D + 1e-06)
        rows[...] = (raw[:, :2048].astype(jnp.float32) * inverse * gain[...]).astype(jnp.bfloat16)
        for base, (step, half) in zip((0, 128), (upper, lower)):
            found = raw[pl.ds(pl.multiple_of(base + lax.rem(me, 8) * 16, 16), 16), :2048]
            here = me // 8 == half
            strip[step] = jnp.where(here, found, strip[step])

    def multiply(step, group, first=False):
        def piece(begin, size):
            for half in range(2):
                value = lax.dot_general(
                    rows[...], weights[half, pl.ds(begin, size), :], (((1,), (1,)), ((), ())),
                    preferred_element_type=jnp.float32,
                )
                parts[step, half, :, pl.ds(begin, size)] = value.astype(jnp.bfloat16)

        if first:
            for n in (range(2), range(2, 8))[group]:
                for copy in weight_copies(n):
                    copy.wait()
        full = 2 if group == 0 else 5

        @pl.loop(0, full)
        def _(n):
            piece(pl.multiple_of(GROUPS[group][0] + n * 256, 256), 256)

        if group == 1:
            piece(1792, 128)

    def cut(ref, sub):
        begin, size = GROUPS[sub % 2]
        return ref.at[:, pl.ds(sub // 2 * 128, 128), pl.ds(begin, size)]

    sent = []

    def part_slot(kind, index):
        return (came_first, came_second)[index].at[kind]

    part_sends = {}

    def pass_part(kind, index, src, way, step):
        at = kind * 2 + index
        copy = remote(src, part_slot(kind, index), psend.at[at], precv.at[at], along_x(way))
        copy.start()
        part_sends.setdefault(step, []).append(copy)

    def part_landed(kind, index):
        at = kind * 2 + index
        landing = part_slot(kind, index)
        remote(landing, landing, psend.at[at], precv.at[at], along_x(1)).wait_recv()
        return landing

    pick(2, True)
    for index in range(2):
        multiply(2, index, True)
        if index == 0:
            greet(plane_neighbours() + [along_x(step) for step in (1, 3)] + [partner()])
        pass_part(0, index, cut(parts.at[2], index), 1, 2)
        pass_part(3, index, cut(parts.at[2], 2 + index), 3, 2)
    pick(1)
    for index in range(2):
        multiply(1, index)
        pass_part(1, index, cut(parts.at[1], index), 1, 1)
        pass_part(4, index, cut(parts.at[1], 2 + index), 3, 1)
    pick(3)
    for index in range(2):
        multiply(3, index)
        for kind, sub, way in ((0, index, 1), (3, 2 + index, 3)):
            arrived = part_landed(kind, index)
            target = cut(parts.at[3], sub)
            target[...] = (target[...].astype(jnp.float32) + arrived[...].astype(jnp.float32)).astype(jnp.bfloat16)
            pass_part(kind + 2, index, target, way, 3)
    pick(0)
    for index in range(2):
        multiply(0, index)

    def hidden_piece(step, sub):
        begin, size = GROUPS[sub % 2]
        return hidden.at[owner(step), pl.ds(sub // 2 * 128, 128), pl.ds(begin, size)]

    def pass_hidden(at, piece, step):
        copy = remote(piece, piece, hsend.at[at], hrecv.at[at], along_x(step))
        copy.start()
        sent.append(copy)

    def hidden_landed(at, piece):
        remote(piece, piece, hsend.at[at], hrecv.at[at], along_x(1)).wait_recv()

    for index in range(2):
        for sub, near, far in ((index, 4, 2), (2 + index, 1, 5)):
            one = part_landed(near, index)
            two = part_landed(far, index)
            own = cut(parts.at[0], sub)
            gate, up = [
                own[half].astype(jnp.float32) + one[half].astype(jnp.float32) + two[half].astype(jnp.float32)
                for half in range(2)
            ]
            piece = hidden_piece(0, sub)
            piece[...] = (gate / (1.0 + jnp.exp(-gate)) * up).astype(jnp.bfloat16)
            pass_hidden(sub, piece, 1)
            pass_hidden(4 + sub, piece, 3)
    for copy in down_copies():
        copy.wait()

    def project(step):
        at = owner(step)
        for copy in part_sends.get(step, []):
            copy.wait_send()
        for side in range(2):
            if side == 1:
                next(flows[step])

            @pl.loop(0, 4)
            def _(n):
                begin = pl.multiple_of(n * 256, 256)
                value = jnp.dot(
                    hidden[at],
                    downs[:, pl.ds(pl.multiple_of(side * 1024 + begin, 256), 256)],
                    preferred_element_type=jnp.float32,
                )
                parts[step, side, :, pl.ds(begin, 256)] = value.astype(jnp.bfloat16)

        next(flows[step])

    def reduction(step):
        def term(t, at):
            return parts.at[step, at // 2, pl.ds(pl.multiple_of(t * 16, 16), 16), pl.ds(at % 2 * 512, 512)]

        def emit(at, value):
            total = value + strip[step, :, pl.ds(at * 512, 512)].astype(jnp.float32)
            target = pl.ds(pl.multiple_of(owner(step) * 16, 16), 16)
            fin[at // 2, target, pl.ds(at % 2 * 512, 512)] = total.astype(jnp.bfloat16)

        return reduce_plane(
            term, got.at[step], made.at[step], sums.at[step], send.at[step], recv.at[step], emit, False
        )

    def relay(index):
        hidden_landed(index, hidden_piece(3, index))
        pass_hidden(8 + index, hidden_piece(3, index), 1)
        hidden_landed(4 + 2 + index, hidden_piece(1, 2 + index))
        pass_hidden(10 + index, hidden_piece(1, 2 + index), 3)

    flows = {step: reduction(step) for step in range(4)}
    project(0)
    relay(0)
    next(flows[0])
    relay(1)
    next(flows[0])
    for index in range(2):
        hidden_landed(2 + index, hidden_piece(3, 2 + index))
    project(3)
    for index in range(2):
        hidden_landed(4 + index, hidden_piece(1, index))
    project(1)
    next(flows[0])
    next(flows[3])
    next(flows[1])
    for index in range(2):
        hidden_landed(8 + index, hidden_piece(2, index))
        hidden_landed(10 + index, hidden_piece(2, 2 + index))
    project(2)
    next(flows[3])
    next(flows[1])
    next(flows[2])
    next(flows[3])
    next(flows[1])
    next(flows[2])
    run(flows[0])
    run(flows[3])
    run(flows[1])
    run(flows[2])
    mine = pl.ds(pl.multiple_of(core * 64, 64), 64)
    theirs = pl.ds(pl.multiple_of((1 - core) * 64, 64), 64)
    swap = remote(fin.at[1 - core], out.at[mine, :], fsend, frecv, partner())
    swap.start()
    out[mine, :] = fin[core]
    swap.wait_send()
    landing = out.at[theirs, :]
    remote(landing, landing, fsend, frecv, partner()).wait_recv()
    for copy in sent + part_sends.get(0, []):
        copy.wait_send()


def feed_forward(everyone, slots, own_gain, other_gain, w_own, w_other, d_own, d_other, collective_id):
    anywhere = pl.BlockSpec(memory_space=pl.ANY)
    vmem = pl.BlockSpec(memory_space=pltpu.VMEM)
    dma = pltpu.SemaphoreType.DMA
    bf16 = jnp.bfloat16
    return pl.pallas_call(
        feed_forward_kernel,
        out_shape=jax.ShapeDtypeStruct((128, 1024), bf16),
        in_specs=[anywhere, vmem, vmem, vmem, anywhere, anywhere, anywhere, anywhere],
        out_specs=vmem,
        scratch_shapes=[
            pltpu.VMEM((2, PADDED, 2048), bf16),
            pltpu.VMEM((PADDED, 2048), bf16),
            pltpu.VMEM((2048, WIDE), bf16),
            pltpu.VMEM((1, 2048), jnp.float32),
            pltpu.VMEM((256, 2048), bf16),
            pltpu.VMEM((256, WIDE), bf16),
            pltpu.VMEM((256, 2048), bf16),
            pltpu.VMEM((4, 16, 2048), bf16),
            pltpu.VMEM((4, 2, 256, PADDED), bf16),
            pltpu.VMEM((6, 2, 128, 512), bf16),
            pltpu.VMEM((6, 2, 128, 1408), bf16),
            pltpu.VMEM((4, 256, PADDED), bf16),
            pltpu.VMEM((4, 60, 16, 512), bf16),
            pltpu.VMEM((4, 20, 16, 512), bf16),
            pltpu.VMEM((4, 16, 16, 512), bf16),
            pltpu.VMEM((2, 64, 1024), bf16),
            dma((9,)),
            dma((8, 2)),
            dma((2,)),
            dma((12,)),
            dma((12,)),
            dma((12,)),
            dma((12,)),
            dma((4, 60)),
            dma((4, 60)),
            dma,
            dma,
        ],
        compiler_params=pltpu.CompilerParams(
            collective_id=collective_id, has_side_effects=True, vmem_limit_bytes=67043328
        ),
        name="feed_forward",
    )(everyone, slots, own_gain, other_gain, w_own, w_other, d_own, d_other)


def local(
    vit_input,
    image_lengths,
    positions,
    vit_ln_gain,
    w_qkv,
    w_proj,
    merger_ln_gain,
    merger_w1,
    merger_w2,
    norm_gain,
    gate_up_weight,
    down_weight,
):
    seq_size = lax.axis_size("seq")
    swap = [(i, i ^ 1) for i in range(seq_size)]
    gate_up_rows = jnp.transpose(gate_up_weight, (1, 2, 0))
    other_rows = lax.ppermute(gate_up_rows, "seq", swap)
    other_down = lax.ppermute(down_weight, "seq", swap)
    other_gain = lax.ppermute(norm_gain, "seq", swap)
    everyone = vision(
        vit_input,
        image_lengths,
        vit_ln_gain,
        merger_ln_gain,
        jnp.transpose(w_qkv, (1, 2, 0)),
        w_proj,
        jnp.transpose(merger_w1),
        merger_w2,
        1,
    ).reshape(-1, WIDE)
    return feed_forward(
        everyone, positions, norm_gain, other_gain, gate_up_rows, other_rows, down_weight, other_down, 2
    )


def solution(mesh):
    finer = Mesh(mesh.devices.reshape(mesh.shape["seq"], 4, 4), ("seq", "tp_0", "tp_1"))
    in_specs = (
        P(SEQ_TP, None),
        P("seq", None),
        P(),
        P(),
        P(None, None, TP),
        P(TP, None),
        P(),
        P(None, TP),
        P(TP, None),
        P("seq"),
        P("seq", None, TP),
        P(TP, "seq"),
    )
    out_specs = P(TP, "seq")
    return jax.shard_map(local, mesh=finer, in_specs=in_specs, out_specs=out_specs, check_vma=False)
```

```python
import jax
import jax.numpy as jnp
from jax import lax
from jax.experimental import pallas as pl
from jax.experimental.pallas import tpu as pltpu
from jax.sharding import Mesh
from jax.sharding import PartitionSpec as P

D = 8192
HD = 80
TP = ("tp_0", "tp_1")
SEQ_TP = ("seq", "tp_0", "tp_1")

MESH_ID = pl.DeviceIdType.MESH
AXES = ("tp_0", "tp_1")


def ring(axis, step):
    return {axis: lax.rem(lax.axis_index(axis) + step, 4)}


def remote(src, dst, send, recv, target):
    return pltpu.make_async_remote_copy(
        src_ref=src, dst_ref=dst, send_sem=send, recv_sem=recv, device_id=target, device_id_type=MESH_ID
    )


def greet(targets):
    barrier = pltpu.get_barrier_semaphore()
    for target in targets:
        pl.semaphore_signal(barrier, inc=1, device_id=target, device_id_type=MESH_ID)
    pl.semaphore_wait(barrier, len(targets))


def plane_neighbours():
    return [ring(axis, step) for axis in AXES for step in (1, 3)]


def gather_plane(own, slot, half_cut, quarter_cut, send, recv, forward=None):
    here = [lax.axis_index(axis) for axis in AXES]
    sent = []

    def index(half, first, second):
        offsets = (first, second) if half == 0 else (second, first)
        spots = [lax.rem(at + off, 4) for at, off in zip(here, offsets)]
        return spots[0] * 4 + spots[1]

    def place(half, first, second):
        return slot(index(half, first, second))

    def source(half, first, second):
        return own if (first, second) == (0, 0) else place(half, first, second)

    def start(half, phase, kind, axis, step, first, second, cut):
        at = half * 20 + phase * 4 + kind
        copy = remote(
            cut(source(half, first, second)), cut(place(half, first, second)), send.at[at], recv.at[at], ring(axis, step)
        )
        copy.start()
        sent.append(copy)

    def landed(half, phase, kind, axis, first, second, cut):
        at = half * 20 + phase * 4 + kind
        target = cut(place(half, first, second))
        remote(target, target, send.at[at], recv.at[at], ring(axis, 1)).wait_recv()
        if forward is not None:
            forward(at, lambda base: cut(base(index(half, first, second))))

    def axes(half):
        return (AXES[0], AXES[1]) if half == 0 else (AXES[1], AXES[0])

    def cuts(half):
        return (
            lambda ref: half_cut(ref, half),
            lambda ref: quarter_cut(ref, 2 * half),
            lambda ref: quarter_cut(ref, 2 * half + 1),
        )

    def spread(half, phase, first):
        whole, _, _ = cuts(half)
        axis = axes(half)[1]
        start(half, phase, 0, axis, 1, first, 0, whole)
        start(half, phase, 1, axis, 3, first, 0, whole)

    def relay(half, phase, first):
        whole, low, high = cuts(half)
        axis = axes(half)[1]
        landed(half, phase, 0, axis, first, 3, whole)
        start(half, phase, 2, axis, 1, first, 3, low)
        landed(half, phase, 1, axis, first, 1, whole)
        start(half, phase, 3, axis, 3, first, 1, high)

    def finish(half, phase, first):
        whole, low, high = cuts(half)
        axis = axes(half)[1]
        landed(half, phase, 2, axis, first, 2, low)
        landed(half, phase, 3, axis, first, 2, high)

    for half in (0, 1):
        whole, _, _ = cuts(half)
        start(half, 0, 0, axes(half)[0], 1, 0, 0, whole)
        start(half, 0, 1, axes(half)[0], 3, 0, 0, whole)
    for half in (0, 1):
        spread(half, 1, 0)
    yield
    for half in (0, 1):
        whole, low, high = cuts(half)
        axis = axes(half)[0]
        landed(half, 0, 0, axis, 3, 0, whole)
        start(half, 0, 2, axis, 1, 3, 0, low)
        spread(half, 2, 3)
        landed(half, 0, 1, axis, 1, 0, whole)
        start(half, 0, 3, axis, 3, 1, 0, high)
        spread(half, 3, 1)
    yield
    for half in (0, 1):
        relay(half, 1, 0)
    yield
    for half in (0, 1):
        whole, low, high = cuts(half)
        axis = axes(half)[0]
        landed(half, 0, 2, axis, 2, 0, low)
        landed(half, 0, 3, axis, 2, 0, high)
        spread(half, 4, 2)
    yield
    for phase, first in ((2, 3), (3, 1), (4, 2)):
        for half in (0, 1):
            relay(half, phase, first)
    yield
    for phase, first in ((1, 0), (2, 3), (3, 1), (4, 2)):
        for half in (0, 1):
            finish(half, phase, first)
    for copy in sent:
        copy.wait_send()


def reduce_plane(term, got, made, sums, send, recv, emit, eager=True):
    here = [lax.axis_index(axis) for axis in AXES]
    sent = []

    def axes(half):
        return (AXES[1], AXES[0]) if half == 0 else (AXES[0], AXES[1])

    def part(half, first, second, which):
        offsets = (first, second) if half == 0 else (second, first)
        spots = [lax.rem(at + off, 4) for at, off in zip(here, offsets)]
        return term(spots[0] * 4 + spots[1], 2 * half + which)

    def phase_source(half, phase):
        if phase < 4:
            return lambda offset, which: part(half, phase, offset, which)
        return lambda offset, which: sums.at[half * 8 + offset * 2 + which]

    def slot(half, phase, kind):
        return half * 30 + phase * 6 + kind

    def start(half, phase, kind, src, step):
        axis = axes(half)[0 if phase < 4 else 1]
        at = slot(half, phase, kind)
        copy = remote(src, got.at[at], send.at[at], recv.at[at], ring(axis, step))
        copy.start()
        sent.append(copy)

    def landed(half, phase, kind):
        at = slot(half, phase, kind)
        axis = axes(half)[0 if phase < 4 else 1]
        remote(got.at[at], got.at[at], send.at[at], recv.at[at], ring(axis, 1)).wait_recv()
        return got[at].astype(jnp.float32)

    def raw(half, phase):
        own = phase_source(half, phase)
        start(half, phase, 0, own(2, 0), 1)
        start(half, phase, 3, own(2, 1), 3)
        start(half, phase, 1, own(1, 1), 1)
        start(half, phase, 4, own(3, 0), 3)

    def summed(half, phase):
        own = phase_source(half, phase)
        for kind, offset, which, step in ((0, 1, 0, 1), (3, 3, 1, 3)):
            at = half * 10 + phase * 2 + which
            made[at] = (own(offset, which)[...].astype(jnp.float32) + landed(half, phase, kind)).astype(made.dtype)
            start(half, phase, kind + 2, made.at[at], step)

    def total(half, phase):
        own = phase_source(half, phase)
        return [
            own(0, which)[...].astype(jnp.float32) + landed(half, phase, near) + landed(half, phase, far)
            for which, near, far in ((0, 4, 2), (1, 1, 5))
        ]

    def settle(half, phase):
        for which, value in enumerate(total(half, phase)):
            sums[half * 8 + phase * 2 + which] = value.astype(sums.dtype)

    order = (2, 1, 3, 0)
    both = (0, 1)

    def late(first):
        own = phase_source_of_last
        for half in both:
            source = own(half)
            if first == 2:
                start(half, 4, 0, source(2, 0), 1)
                start(half, 4, 3, source(2, 1), 3)
            if first == 1:
                start(half, 4, 1, source(1, 1), 1)
            if first == 3:
                start(half, 4, 4, source(3, 0), 3)

    def phase_source_of_last(half):
        return phase_source(half, 4)

    for half in both:
        for phase in order[:2] if eager else order:
            raw(half, phase)
        yield
    for at, phase in enumerate(order):
        for half in both:
            summed(half, phase)
        if eager and at + 2 < 4:
            for half in both:
                raw(half, order[at + 2])
        if eager and at >= 1:
            for half in both:
                settle(half, order[at - 1])
            late(order[at - 1])
    yield
    if not eager:
        for phase in order[:3]:
            for half in both:
                settle(half, phase)
            late(phase)
    yield
    for half in both:
        summed(half, 4)
    yield
    for half in both:
        settle(half, 0)
    for half in both:
        for which, value in enumerate(total(half, 4)):
            emit(2 * half + which, value)
    for copy in sent:
        copy.wait_send()


def run(steps):
    for _ in steps:
        pass
WIDE = 2176
PADDED = 1920


def along_x(step):
    seq = lax.axis_index("seq")
    return {"seq": lax.rem(seq + 2 * step, 8)}


def partner():
    seq = lax.axis_index("seq")
    return {"seq": seq + 1 - 2 * lax.rem(seq, 2)}


ROW_CUTS = ((0, 32), (32, 16), (48, 16), (64, 16))
ROW_HALVES = ((0, 48), (48, 32))


def share_with_partner(buffer, core, send, recv, sent, expected):
    def forward(at, view):
        piece = view(lambda t: buffer(core, t))
        copy = remote(piece, piece, send.at[at], recv.at[at], partner())
        copy.start()
        sent.append(copy)
        other = view(lambda t: buffer(1 - core, t))
        expected.append(remote(other, other, send.at[at], recv.at[at], partner()))

    return forward


def norm_rows(values, gain):
    mean = jnp.mean(values, axis=-1, keepdims=True)
    centered = values - mean
    variance = jnp.mean(centered * centered, axis=-1, keepdims=True)
    return centered * lax.rsqrt(variance + 1e-06) * gain


def vision_kernel(
    vit, ends, ln_gain, merger_gain, w_qkv, w_proj, w_one, w_two, out,
    own, patches, qkv, wq, wp, att, heads, lined, tiles, block_in, merged, one, expanded, two, terms,
    got, made, sums, parcels,
    wsem, asend, arecv, psend, precv, qsend, qrecv, hsend, hrecv, msend, mrecv,
    send, recv, xsend, xrecv,
):
    seq = lax.axis_index("seq")
    x, core = seq // 2, lax.rem(seq, 2)
    y, z = [lax.axis_index(axis) for axis in AXES]
    me = y * 4 + z
    others = [(dy, dz) for dy in range(4) for dz in range(4) if (dy, dz) != (0, 0)]

    def peer(dy, dz):
        return {"tp_0": lax.rem(y + dy, 4), "tp_1": lax.rem(z + dz, 4)}

    def peer_index(dy, dz):
        return lax.rem(y + dy, 4) * 4 + lax.rem(z + dz, 4)

    def proj_slot(side, t):
        return wp.at[t, :, pl.ds(pl.multiple_of(side * 640, 128), 640)]

    wq[:, pl.ds(80, 48), :] = jnp.zeros((3, 48, 1280), jnp.bfloat16)
    loads = [
        pltpu.make_async_copy(w_qkv, wq.at[:, pl.ds(0, 80), :], wsem.at[0]),
        pltpu.make_async_copy(w_proj, wp.at[me], wsem.at[1]),
        pltpu.make_async_copy(w_one, one, wsem.at[2]),
        pltpu.make_async_copy(w_two, two, wsem.at[3]),
    ]
    for copy in loads[:2]:
        copy.start()
    targets = [peer(*offset) for offset in others] + [along_x(step) for step in (1, 2, 3)] + [partner()]
    barrier = pltpu.get_barrier_semaphore()
    for target in targets:
        pl.semaphore_signal(barrier, inc=1, device_id=target, device_id_type=MESH_ID)
    own[...] = norm_rows(vit[...].astype(jnp.float32), ln_gain[...][None]).astype(jnp.bfloat16)
    pl.semaphore_wait(barrier, len(targets))

    rows_half = lambda ref, half: ref.at[pl.ds(half * 32, 32), :]
    rows_quarter = lambda ref, at: ref.at[pl.ds(at * 16, 16), :]
    patches[me] = own[...]
    arrive = gather_plane(own, lambda t: patches.at[t], rows_half, rows_quarter, asend, arecv)
    next(arrive)
    loads[1].wait()
    shared, awaited = [], []
    weights = gather_plane(
        proj_slot(core, me),
        lambda t: proj_slot(core, t),
        lambda ref, half: ref.at[pl.ds(*ROW_HALVES[half]), :],
        lambda ref, at: ref.at[pl.ds(*ROW_CUTS[at]), :],
        psend,
        precv,
        share_with_partner(proj_slot, core, qsend, qrecv, shared, awaited),
    )
    next(weights)
    next(arrive)
    loads[2].start()
    next(arrive)
    next(arrive)
    next(weights)
    loads[3].start()
    next(arrive)
    next(weights)
    run(arrive)
    loads[0].wait()

    @pl.loop(0, 4)
    def _(n):
        rows = pl.ds(pl.multiple_of(n * 256, 256), 256)
        some = patches[pl.ds(n * 4, 4)].reshape(256, 1280)
        for which in range(3):
            qkv[which, rows, :] = lax.dot_general(
                some, wq[which], (((1,), (1,)), ((), ())), preferred_element_type=jnp.float32
            ).astype(jnp.bfloat16)

    next(weights)
    end = ends[0:1, 0:1] * 4

    def attend_rows(n):
        rows = pl.ds(pl.multiple_of(n * 256, 256), 256)
        scores = lax.dot_general(
            qkv[0, rows, :], qkv[1], (((1,), (1,)), ((), ())), preferred_element_type=jnp.float32
        ) * HD ** (-0.5)
        query_first = n * 256 + lax.broadcasted_iota(jnp.int32, (256, 1), 0) < end
        key_first = lax.broadcasted_iota(jnp.int32, (1, 1024), 1) < end
        query_first = jnp.where(query_first, 1, 0)
        key_first = jnp.where(key_first, 1, 0)
        scores = jnp.where(query_first == key_first, scores, -1e30)
        top = jnp.max(scores, axis=-1, keepdims=True)
        expo = jnp.exp(scores - top)
        share = (expo / jnp.sum(expo, axis=-1, keepdims=True)).astype(jnp.bfloat16)
        mixed = jnp.dot(share, qkv[2], preferred_element_type=jnp.float32).astype(jnp.bfloat16)
        att[pl.ds(n * 4, 4)] = mixed.reshape(4, 64, 128)

    for n in range(2):
        @pl.loop(2 * n, 2 * n + 2)
        def _(at):
            attend_rows(at)

        if n == 0:
            next(weights)
    sent = []
    for at, offset in enumerate(others):
        copy = remote(att.at[peer_index(*offset)], heads.at[me], hsend.at[at], hrecv.at[at], peer(*offset))
        copy.start()
        sent.append(copy)
    heads[me] = att[me]
    run(weights)
    for copy in shared:
        copy.wait_send()
    for copy in awaited:
        copy.wait_recv()
    for at, (dy, dz) in enumerate(others):
        landing = heads.at[peer_index(4 - dy, 4 - dz)]
        remote(landing, landing, hsend.at[at], hrecv.at[at], peer(dy, dz)).wait_recv()
    for copy in sent:
        copy.wait_send()
    lined[...] = vit[...].astype(jnp.float32)

    @pl.loop(0, 16)
    def _(head):
        lined[...] += jnp.dot(heads[head, :, :80], wp[head], preferred_element_type=jnp.float32)

    ready = norm_rows(lined[...], merger_gain[...][None])
    for tile in range(10):
        tiles[tile] = ready[:, tile * 128 : tile * 128 + 128]
    for at in range(4):
        for tile in range(10):
            strided = tiles[tile, pl.ds(at, 16, stride=4), :]
            block_in[:, pl.ds(at * 1280 + tile * 128, 128)] = strided.astype(jnp.bfloat16)
    merged[pl.ds(pl.multiple_of(me * 16, 16), 16), :] = block_in[...]
    run(gather_plane(
        block_in,
        lambda t: merged.at[pl.ds(pl.multiple_of(t * 16, 16), 16), :],
        lambda ref, half: ref.at[:, pl.ds(half * 2560, 2560)],
        lambda ref, at: ref.at[:, pl.ds(at * 1280, 1280)],
        msend,
        mrecv,
    ))
    loads[2].wait()
    total = lax.dot_general(
        merged[...], one[...], (((1,), (1,)), ((), ())), preferred_element_type=jnp.float32
    )
    expanded[...] = (0.5 * total * (1.0 + lax.erf(total * (0.5 ** 0.5)))).astype(jnp.bfloat16)
    loads[3].wait()

    def share_of(half):
        @pl.loop(8 * half, 8 * half + 8)
        def _(n):
            columns = pl.ds(pl.multiple_of(n * 512, 512), 512)
            terms[:, columns] = jnp.dot(
                expanded[...], two[:, columns], preferred_element_type=jnp.float32
            ).astype(jnp.bfloat16)

    def emit(at, value):
        parcels[at, :, :2048] = value.astype(jnp.bfloat16)

    def term(t, at):
        return terms.at[pl.ds(pl.multiple_of(t * 16, 16), 16), pl.ds(at * 2048, 2048)]

    shares = reduce_plane(term, got, made, sums, send, recv, emit)
    share_of(0)
    next(shares)
    share_of(1)
    run(shares)
    squares = jnp.zeros((16, 1), jnp.float32)
    for at in range(4):
        values = parcels[at, :, :2048].astype(jnp.float32)
        squares = squares + jnp.sum(values * values, axis=1, keepdims=True)
    high = squares.astype(jnp.bfloat16).astype(jnp.float32)
    low = squares - high
    lane = lax.broadcasted_iota(jnp.int32, (16, 128), 1)
    tail = jnp.where(lane == 0, high, jnp.where(lane == 1, low, 0.0)).astype(jnp.bfloat16)
    for at in range(4):
        parcels[at, :, 2048:] = tail
    sent = []
    for step in (2, 1, 3):
        copy = remote(
            parcels.at[lax.rem(x + step, 4)], out.at[x], xsend.at[step], xrecv.at[step], along_x(step)
        )
        copy.start()
        sent.append(copy)
    out[x] = parcels[x]
    for step in (1, 3, 2):
        landing = out.at[lax.rem(x + 4 - step, 4)]
        remote(landing, landing, xsend.at[step], xrecv.at[step], along_x(step)).wait_recv()
    for copy in sent:
        copy.wait_send()


def vision(vit, ends, ln_gain, merger_gain, w_qkv, w_proj, w_one, w_two, collective_id):
    anywhere = pl.BlockSpec(memory_space=pl.ANY)
    vmem = pl.BlockSpec(memory_space=pltpu.VMEM)
    dma = pltpu.SemaphoreType.DMA
    bf16 = jnp.bfloat16
    return pl.pallas_call(
        vision_kernel,
        out_shape=jax.ShapeDtypeStruct((4, 16, WIDE), bf16),
        in_specs=[vmem] * 4 + [anywhere] * 4,
        out_specs=vmem,
        scratch_shapes=[
            pltpu.VMEM((64, 1280), bf16),
            pltpu.VMEM((16, 64, 1280), bf16),
            pltpu.VMEM((3, 1024, 128), bf16),
            pltpu.VMEM((3, 128, 1280), bf16),
            pltpu.VMEM((16, 80, 1280), bf16),
            pltpu.VMEM((16, 64, 128), bf16),
            pltpu.VMEM((16, 64, 128), bf16),
            pltpu.VMEM((64, 1280), jnp.float32),
            pltpu.VMEM((10, 64, 128), jnp.float32),
            pltpu.VMEM((16, 5120), bf16),
            pltpu.VMEM((256, 5120), bf16),
            pltpu.VMEM((320, 5120), bf16),
            pltpu.VMEM((256, 320), bf16),
            pltpu.VMEM((320, 8192), bf16),
            pltpu.VMEM((256, 8192), bf16),
            pltpu.VMEM((60, 16, 2048), bf16),
            pltpu.VMEM((20, 16, 2048), bf16),
            pltpu.VMEM((16, 16, 2048), bf16),
            pltpu.VMEM((4, 16, WIDE), bf16),
            dma((4,)),
            dma((40,)), dma((40,)),
            dma((40,)), dma((40,)),
            dma((40,)), dma((40,)),
            dma((15,)), dma((15,)),
            dma((40,)), dma((40,)),
            dma((60,)), dma((60,)),
            dma((4,)), dma((4,)),
        ],
        compiler_params=pltpu.CompilerParams(
            collective_id=collective_id, has_side_effects=True, vmem_limit_bytes=56 * 1024 * 1024
        ),
        name="vision",
    )(vit, ends, ln_gain, merger_gain, w_qkv, w_proj, w_one, w_two)


GROUPS = ((0, 512), (512, 1408))
BLOCKS = (((0, 0), (0, 1)), ((1, 1), (3, 0)), ((2, 0), (2, 1)), ((1, 0), (3, 1)))


def feed_forward_kernel(
    block, slots, own_gain, other_gain, w_own, w_other, d_own, d_other, out,
    weights, downs, everyone, gain, seats, picks, raw, rows, strip, parts, came_first, came_second, hidden, got, made, sums, fin,
    gsend, grecv, dsend, drecv, wsem, osem, psend, precv, hsend, hrecv, send, recv, fsend, frecv,
):
    seq = lax.axis_index("seq")
    x, core = seq // 2, lax.rem(seq, 2)
    me = lax.axis_index("tp_0") * 4 + lax.axis_index("tp_1")
    real = w_own.shape[1]
    first_core = core == 0
    gain[:, :1024] = jnp.where(first_core, own_gain[...], other_gain[...])[None]
    gain[:, 1024:] = jnp.where(first_core, other_gain[...], own_gain[...])[None]
    weights[:, pl.ds(1840, 80), :] = jnp.zeros((2, 80, 2048), jnp.bfloat16)
    downs[pl.ds(1840, 80), :] = jnp.zeros((80, 2048), jnp.bfloat16)
    sides = ((w_own, d_own, core), (w_other, d_other, 1 - core))

    def weight_copies(n):
        size = 256 if n < 7 else real - 1792
        return [
            pltpu.make_async_copy(
                w.at[:, pl.ds(n * 256, size), :],
                weights.at[:, pl.ds(n * 256, size), pl.ds(pl.multiple_of(at * 1024, 1024), 1024)],
                wsem.at[n, side],
            )
            for side, (w, _, at) in enumerate(sides)
        ]

    def down_copies():
        return [
            pltpu.make_async_copy(
                d, downs.at[pl.ds(0, real), pl.ds(pl.multiple_of(at * 1024, 1024), 1024)], osem.at[side]
            )
            for side, (_, d, at) in enumerate(sides)
        ]

    strip[...] = jnp.zeros_like(strip)

    def owner(step):
        return lax.rem(x + step, 4)

    greet(plane_neighbours() + [along_x(step) for step in (1, 3)] + [partner()])
    forwarded, expected = [], []

    def spot(side, t):
        return everyone.at[:, side, t]

    own_copy = remote(block, spot(core, me), dsend.at[40], drecv.at[40], partner())
    own_copy.start()
    everyone[:, core, me] = block[...]
    arrive = gather_plane(
        block,
        lambda t: spot(core, t),
        lambda ref, half: ref.at[pl.ds(half * 2, 2)],
        lambda ref, at: ref.at[pl.ds(at, 1)],
        gsend,
        grecv,
        share_with_partner(spot, core, dsend, drecv, forwarded, expected),
    )
    for turn in range(4):
        next(arrive)
        for n in (2 * turn, 2 * turn + 1):
            for copy in weight_copies(n):
                copy.start()
    run(arrive)
    other = spot(1 - core, me)
    expected.append(remote(other, other, dsend.at[40], drecv.at[40], partner()))
    seats_of_all = slots[...][None]
    for side in range(2):
        for at in range(4):
            begin = at * 512 + side * 256
            seats[side, :, pl.ds(at * 256, 256)] = seats_of_all[:, begin : begin + 256]

    def pick(step, first=False):
        upper, lower = BLOCKS[step]
        row = lax.broadcasted_iota(jnp.int32, (256, 1), 0)
        top = row < 128
        at = jnp.where(top, owner(upper[0]), owner(lower[0]))
        row = jnp.where(top, row + upper[1] * 128, row - 128 + lower[1] * 128)
        slot = (row // 16) * 128 + core * 64 + at * 16 + row % 16
        for at, side in enumerate((core, 1 - core)):
            picks[at] = jnp.where(seats[side] == slot, 1.0, 0.0).astype(jnp.bfloat16)

        def found(at, columns):
            side = core if at == 0 else 1 - core
            some = everyone[:, side, :, :, columns].reshape(1024, columns.size)
            return jnp.dot(picks[at], some, preferred_element_type=jnp.float32)

        def over_columns(fill):
            @pl.loop(0, 8)
            def _(n):
                fill(pl.ds(pl.multiple_of(n * 256, 256), 256))

            fill(pl.ds(2048, 128))

        def fill_own(columns):
            raw[:, columns] = found(0, columns).astype(jnp.bfloat16)

        def fill_other(columns):
            raw[:, columns] = (raw[:, columns].astype(jnp.float32) + found(1, columns)).astype(jnp.bfloat16)

        def fill_both(columns):
            raw[:, columns] = (found(0, columns) + found(1, columns)).astype(jnp.bfloat16)

        if first:
            over_columns(fill_own)
            for copy in expected:
                copy.wait_recv()
            own_copy.wait_send()
            for copy in forwarded:
                copy.wait_send()
            over_columns(fill_other)
        else:
            over_columns(fill_both)
        square = raw[:, 2048:2049].astype(jnp.float32) + raw[:, 2049:2050].astype(jnp.float32)
        inverse = lax.rsqrt(square / D + 1e-06)
        rows[...] = (raw[:, :2048].astype(jnp.float32) * inverse * gain[...]).astype(jnp.bfloat16)
        for base, (step, half) in zip((0, 128), (upper, lower)):
            found = raw[pl.ds(pl.multiple_of(base + lax.rem(me, 8) * 16, 16), 16), :2048]
            here = me // 8 == half
            strip[step] = jnp.where(here, found, strip[step])

    def multiply(step, group, first=False):
        def piece(begin, size):
            for half in range(2):
                value = lax.dot_general(
                    rows[...], weights[half, pl.ds(begin, size), :], (((1,), (1,)), ((), ())),
                    preferred_element_type=jnp.float32,
                )
                parts[step, half, :, pl.ds(begin, size)] = value.astype(jnp.bfloat16)

        if first:
            for n in (range(2), range(2, 8))[group]:
                for copy in weight_copies(n):
                    copy.wait()
        full = 2 if group == 0 else 5

        @pl.loop(0, full)
        def _(n):
            piece(pl.multiple_of(GROUPS[group][0] + n * 256, 256), 256)

        if group == 1:
            piece(1792, 128)

    def cut(ref, sub):
        begin, size = GROUPS[sub % 2]
        return ref.at[:, pl.ds(sub // 2 * 128, 128), pl.ds(begin, size)]

    sent = []

    def part_slot(kind, index):
        return (came_first, came_second)[index].at[kind]

    part_sends = {}

    def pass_part(kind, index, src, way, step):
        at = kind * 2 + index
        copy = remote(src, part_slot(kind, index), psend.at[at], precv.at[at], along_x(way))
        copy.start()
        part_sends.setdefault(step, []).append(copy)

    def part_landed(kind, index):
        at = kind * 2 + index
        landing = part_slot(kind, index)
        remote(landing, landing, psend.at[at], precv.at[at], along_x(1)).wait_recv()
        return landing

    pick(2, True)
    for index in range(2):
        multiply(2, index, True)
        pass_part(0, index, cut(parts.at[2], index), 1, 2)
        pass_part(3, index, cut(parts.at[2], 2 + index), 3, 2)
    pick(1)
    for index in range(2):
        multiply(1, index)
        pass_part(1, index, cut(parts.at[1], index), 1, 1)
        pass_part(4, index, cut(parts.at[1], 2 + index), 3, 1)
    pick(3)
    for index in range(2):
        multiply(3, index)
        for kind, sub, way in ((0, index, 1), (3, 2 + index, 3)):
            arrived = part_landed(kind, index)
            target = cut(parts.at[3], sub)
            target[...] = (target[...].astype(jnp.float32) + arrived[...].astype(jnp.float32)).astype(jnp.bfloat16)
            pass_part(kind + 2, index, target, way, 3)
    for copy in down_copies():
        copy.start()
    pick(0)
    for index in range(2):
        multiply(0, index)

    def hidden_piece(step, sub):
        begin, size = GROUPS[sub % 2]
        return hidden.at[owner(step), pl.ds(sub // 2 * 128, 128), pl.ds(begin, size)]

    def pass_hidden(at, piece, step):
        copy = remote(piece, piece, hsend.at[at], hrecv.at[at], along_x(step))
        copy.start()
        sent.append(copy)

    def hidden_landed(at, piece):
        remote(piece, piece, hsend.at[at], hrecv.at[at], along_x(1)).wait_recv()

    for index in range(2):
        for sub, near, far in ((index, 4, 2), (2 + index, 1, 5)):
            one = part_landed(near, index)
            two = part_landed(far, index)
            own = cut(parts.at[0], sub)
            gate, up = [
                own[half].astype(jnp.float32) + one[half].astype(jnp.float32) + two[half].astype(jnp.float32)
                for half in range(2)
            ]
            piece = hidden_piece(0, sub)
            piece[...] = (gate / (1.0 + jnp.exp(-gate)) * up).astype(jnp.bfloat16)
            pass_hidden(sub, piece, 1)
            pass_hidden(4 + sub, piece, 3)
    for copy in down_copies():
        copy.wait()

    def project(step):
        at = owner(step)
        for copy in part_sends.get(step, []):
            copy.wait_send()
        for side in range(2):
            if side == 1:
                next(flows[step])

            @pl.loop(0, 4)
            def _(n):
                begin = pl.multiple_of(n * 256, 256)
                value = jnp.dot(
                    hidden[at],
                    downs[:, pl.ds(pl.multiple_of(side * 1024 + begin, 256), 256)],
                    preferred_element_type=jnp.float32,
                )
                parts[step, side, :, pl.ds(begin, 256)] = value.astype(jnp.bfloat16)

        next(flows[step])

    def reduction(step):
        def term(t, at):
            return parts.at[step, at // 2, pl.ds(pl.multiple_of(t * 16, 16), 16), pl.ds(at % 2 * 512, 512)]

        def emit(at, value):
            total = value + strip[step, :, pl.ds(at * 512, 512)].astype(jnp.float32)
            target = pl.ds(pl.multiple_of(owner(step) * 16, 16), 16)
            fin[at // 2, target, pl.ds(at % 2 * 512, 512)] = total.astype(jnp.bfloat16)

        return reduce_plane(
            term, got.at[step], made.at[step], sums.at[step], send.at[step], recv.at[step], emit, False
        )

    def relay(index):
        hidden_landed(index, hidden_piece(3, index))
        pass_hidden(8 + index, hidden_piece(3, index), 1)
        hidden_landed(4 + 2 + index, hidden_piece(1, 2 + index))
        pass_hidden(10 + index, hidden_piece(1, 2 + index), 3)

    flows = {step: reduction(step) for step in range(4)}
    project(0)
    relay(0)
    next(flows[0])
    relay(1)
    next(flows[0])
    for index in range(2):
        hidden_landed(2 + index, hidden_piece(3, 2 + index))
    project(3)
    for index in range(2):
        hidden_landed(4 + index, hidden_piece(1, index))
    project(1)
    next(flows[0])
    next(flows[3])
    next(flows[1])
    for index in range(2):
        hidden_landed(8 + index, hidden_piece(2, index))
        hidden_landed(10 + index, hidden_piece(2, 2 + index))
    project(2)
    next(flows[3])
    next(flows[1])
    next(flows[2])
    next(flows[3])
    next(flows[1])
    next(flows[2])
    run(flows[0])
    run(flows[3])
    run(flows[1])
    run(flows[2])
    mine = pl.ds(pl.multiple_of(core * 64, 64), 64)
    theirs = pl.ds(pl.multiple_of((1 - core) * 64, 64), 64)
    swap = remote(fin.at[1 - core], out.at[mine, :], fsend, frecv, partner())
    swap.start()
    out[mine, :] = fin[core]
    swap.wait_send()
    landing = out.at[theirs, :]
    remote(landing, landing, fsend, frecv, partner()).wait_recv()
    for copy in sent + part_sends.get(0, []):
        copy.wait_send()


def feed_forward(block, slots, own_gain, other_gain, w_own, w_other, d_own, d_other, collective_id):
    anywhere = pl.BlockSpec(memory_space=pl.ANY)
    vmem = pl.BlockSpec(memory_space=pltpu.VMEM)
    dma = pltpu.SemaphoreType.DMA
    bf16 = jnp.bfloat16
    return pl.pallas_call(
        feed_forward_kernel,
        out_shape=jax.ShapeDtypeStruct((128, 1024), bf16),
        in_specs=[vmem, vmem, vmem, vmem, anywhere, anywhere, anywhere, anywhere],
        out_specs=vmem,
        scratch_shapes=[
            pltpu.VMEM((2, PADDED, 2048), bf16),
            pltpu.VMEM((PADDED, 2048), bf16),
            pltpu.VMEM((4, 2, 16, 16, WIDE), bf16),
            pltpu.VMEM((1, 2048), jnp.float32),
            pltpu.VMEM((2, 1, 1024), jnp.int32),
            pltpu.VMEM((2, 256, 1024), bf16),
            pltpu.VMEM((256, WIDE), bf16),
            pltpu.VMEM((256, 2048), bf16),
            pltpu.VMEM((4, 16, 2048), bf16),
            pltpu.VMEM((4, 2, 256, PADDED), bf16),
            pltpu.VMEM((6, 2, 128, 512), bf16),
            pltpu.VMEM((6, 2, 128, 1408), bf16),
            pltpu.VMEM((4, 256, PADDED), bf16),
            pltpu.VMEM((4, 60, 16, 512), bf16),
            pltpu.VMEM((4, 20, 16, 512), bf16),
            pltpu.VMEM((4, 16, 16, 512), bf16),
            pltpu.VMEM((2, 64, 1024), bf16),
            dma((40,)),
            dma((40,)),
            dma((41,)),
            dma((41,)),
            dma((8, 2)),
            dma((2,)),
            dma((12,)),
            dma((12,)),
            dma((12,)),
            dma((12,)),
            dma((4, 60)),
            dma((4, 60)),
            dma,
            dma,
        ],
        compiler_params=pltpu.CompilerParams(
            collective_id=collective_id, has_side_effects=True, vmem_limit_bytes=67043328
        ),
        name="feed_forward",
    )(block, slots, own_gain, other_gain, w_own, w_other, d_own, d_other)


def local(
    vit_input,
    image_lengths,
    positions,
    vit_ln_gain,
    w_qkv,
    w_proj,
    merger_ln_gain,
    merger_w1,
    merger_w2,
    norm_gain,
    gate_up_weight,
    down_weight,
):
    seq_size = lax.axis_size("seq")
    swap = [(i, i ^ 1) for i in range(seq_size)]
    gate_up_rows = jnp.transpose(gate_up_weight, (1, 2, 0))
    other_rows = lax.ppermute(gate_up_rows, "seq", swap)
    other_down = lax.ppermute(down_weight, "seq", swap)
    other_gain = lax.ppermute(norm_gain, "seq", swap)
    block = vision(
        vit_input,
        image_lengths,
        vit_ln_gain,
        merger_ln_gain,
        jnp.transpose(w_qkv, (1, 2, 0)),
        w_proj,
        jnp.transpose(merger_w1),
        merger_w2,
        1,
    )
    return feed_forward(
        block, positions, norm_gain, other_gain, gate_up_rows, other_rows, down_weight, other_down, 2
    )


def solution(mesh):
    finer = Mesh(mesh.devices.reshape(mesh.shape["seq"], 4, 4), ("seq", "tp_0", "tp_1"))
    in_specs = (
        P(SEQ_TP, None),
        P("seq", None),
        P(),
        P(),
        P(None, None, TP),
        P(TP, None),
        P(),
        P(None, TP),
        P(TP, None),
        P("seq"),
        P("seq", None, TP),
        P(TP, "seq"),
    )
    out_specs = P(TP, "seq")
    return jax.shard_map(local, mesh=finer, in_specs=in_specs, out_specs=out_specs, check_vma=False)
```
